32 devices in a mesh: dp: 4 (over z), tp: 8 (over y, x, core).
Axes of the slice: x: 2, y: 2, z: 4, core: 2. Of those that a mesh axis runs over, the one named last changes fastest.
Arguments:
- hidden: bfloat16 [512, 1536], P('dp'), parts along dimension 0
- tokens: int32 [512], P('dp'), parts along dimension 0
- embedding: bfloat16 [151936, 1536], P('tp')
- head_w: bfloat16 [1536, 151936], P(None, 'tp')
- h_norm: float32 [1536], replicated
- e_norm: float32 [1536], replicated
- f_norm: float32 [1536], replicated
- o_norm: float32 [1536], replicated
- proj_w: bfloat16 [3072, 1536], P(None, 'tp')
- w_gate: bfloat16 [1536, 8960], P(None, 'tp')
- w_up: bfloat16 [1536, 8960], P(None, 'tp')
- w_down: bfloat16 [8960, 1536], P('tp')
Outputs:
- output 1: bfloat16 [512, 1536], P('dp'), parts along dimension 0
- output 2: float32 [512, 151936], P('dp', 'tp'), parts along dimension 0
There are 4 independent parts. The reference program is written for one: setup_inputs(seed, part) draws one part's arguments, and reference() takes and returns one part's arrays. A program takes and returns all parts, laid end to end along the dimension named above; an argument that names none is the same for every part.
All inputs are finite; a program needn't handle non-finite values.
Results may differ from the reference program's by a relative error of at most 0.0111825.
Values are sent between devices in bfloat16 or wider.
A program may use at most 1 GiB of HBM per device.

```python
import jax
import jax.numpy as jnp
from jax import lax

MODEL_DIM = 1536
VOCAB_SIZE = 151936
FFN_DIM = 8960
BATCH_ROWS = 128

HOT_WIDTH = VOCAB_SIZE // 32
NORM_EPS = 1e-6


def draw_tokens(key_in):
    sub_keys = jax.random.split(key_in, 4)
    hot_starts = jax.random.randint(sub_keys[0], (2,), 0, VOCAB_SIZE - HOT_WIDTH + 1)
    choice = jax.random.randint(sub_keys[1], (BATCH_ROWS,), 0, 4)
    offsets = jax.random.randint(sub_keys[2], (BATCH_ROWS,), 0, HOT_WIDTH)
    spread = jax.random.randint(sub_keys[3], (BATCH_ROWS,), 0, VOCAB_SIZE)
    hot_ids = jnp.where(choice == 3, hot_starts[1], hot_starts[0]) + offsets
    token_ids = jnp.where(choice == 0, spread, hot_ids)
    return token_ids.at[0].set(0).at[BATCH_ROWS - 1].set(VOCAB_SIZE - 1).astype(jnp.int32)


def setup_inputs(seed: int = 0, part: int = 0) -> dict:
    root_key = jax.random.key(seed)
    part_keys = jax.random.split(jax.random.fold_in(root_key, part), 2)
    weight_keys = jax.random.split(root_key, 10)
    hidden = (2.0 * jax.random.normal(part_keys[0], (BATCH_ROWS, MODEL_DIM), jnp.float32)).astype(jnp.bfloat16)
    tokens = draw_tokens(part_keys[1])
    embedding = jax.random.normal(weight_keys[0], (VOCAB_SIZE, MODEL_DIM), jnp.float32).astype(jnp.bfloat16)
    head_w = (jax.random.normal(weight_keys[1], (MODEL_DIM, VOCAB_SIZE), jnp.float32) * (1.5 * MODEL_DIM ** -0.5)).astype(jnp.bfloat16)
    h_norm = 1.0 + 0.5 * jax.random.normal(weight_keys[2], (MODEL_DIM,), jnp.float32)
    e_norm = 1.0 + 0.5 * jax.random.normal(weight_keys[3], (MODEL_DIM,), jnp.float32)
    f_norm = 1.0 + 0.5 * jax.random.normal(weight_keys[4], (MODEL_DIM,), jnp.float32)
    o_norm = 1.0 + 0.5 * jax.random.normal(weight_keys[5], (MODEL_DIM,), jnp.float32)
    proj_w = (jax.random.normal(weight_keys[6], (2 * MODEL_DIM, MODEL_DIM), jnp.float32) * (2 * MODEL_DIM) ** -0.5).astype(jnp.bfloat16)
    w_gate = (jax.random.normal(weight_keys[7], (MODEL_DIM, FFN_DIM), jnp.float32) * MODEL_DIM ** -0.5).astype(jnp.bfloat16)
    w_up = (jax.random.normal(weight_keys[8], (MODEL_DIM, FFN_DIM), jnp.float32) * MODEL_DIM ** -0.5).astype(jnp.bfloat16)
    w_down = (jax.random.normal(weight_keys[9], (FFN_DIM, MODEL_DIM), jnp.float32) * FFN_DIM ** -0.5).astype(jnp.bfloat16)
    return {"hidden": hidden, "tokens": tokens, "embedding": embedding, "head_w": head_w, "h_norm": h_norm, "e_norm": e_norm, "f_norm": f_norm, "o_norm": o_norm, "proj_w": proj_w, "w_gate": w_gate, "w_up": w_up, "w_down": w_down}


def rms_norm(values, norm_gain):
    wide_vals = values.astype(jnp.float32)
    inv_rms = lax.rsqrt(jnp.mean(wide_vals * wide_vals, axis=-1, keepdims=True) + NORM_EPS)
    return wide_vals * inv_rms * norm_gain


def reference(hidden, tokens, embedding, head_w, h_norm, e_norm, f_norm, o_norm, proj_w, w_gate, w_up, w_down):
    emb_rows = jnp.take(embedding, tokens, axis=0)
    joined = jnp.concatenate([rms_norm(hidden, h_norm), rms_norm(emb_rows, e_norm)], axis=-1).astype(jnp.bfloat16)
    proj_full = jnp.dot(joined, proj_w, preferred_element_type=jnp.float32).astype(jnp.bfloat16)
    normed = rms_norm(proj_full, f_norm).astype(jnp.bfloat16)
    gate_val = jnp.dot(normed, w_gate, preferred_element_type=jnp.float32)
    up_val = jnp.dot(normed, w_up, preferred_element_type=jnp.float32)
    act_val = (jax.nn.silu(gate_val) * up_val).astype(jnp.bfloat16)
    down_val = jnp.dot(act_val, w_down, preferred_element_type=jnp.float32)
    new_u = (proj_full.astype(jnp.float32) + down_val).astype(jnp.bfloat16)
    out_norm = rms_norm(new_u, o_norm).astype(jnp.bfloat16)
    logits = jnp.dot(out_norm, head_w, preferred_element_type=jnp.float32)
    log_total = jax.nn.logsumexp(logits, axis=-1, keepdims=True)
    return new_u, logits - log_total
```

```python
import functools

import jax
import jax.numpy as jnp
from jax import lax
from jax.experimental import pallas as pl
from jax.experimental.pallas import tpu as pltpu
from jax.sharding import PartitionSpec as P

NORM_EPS = 1e-6
TILE = 512
SLOTS = 23
MESH = pl.DeviceIdType.MESH
F32, BF16 = jnp.float32, jnp.bfloat16


def rms(values, gain, axis):
    wide = values.astype(F32)
    inv = lax.rsqrt(jnp.mean(wide * wide, axis=axis, keepdims=True) + NORM_EPS)
    return wide * inv * gain


def dot_t(a, b):
    return lax.dot_general(a, b, (((1,), (1,)), ((), ())), preferred_element_type=F32)


def gather_kernel(ids_ref, ids_row_ref, emb_ref, out_ref, buf, sem):
    rows, vocab = out_ref.shape[0], emb_ref.shape[0]
    base = lax.axis_index("tp") * vocab

    def issue(r, carry):
        local = jnp.clip(ids_ref[r] - base, 0, vocab - 1)
        start = pl.multiple_of((local // 8) * 8, 8)
        pltpu.make_async_copy(emb_ref.at[pl.ds(start, 8), :], buf.at[pl.ds(pl.multiple_of(r * 8, 8), 8), :], sem).start()
        return carry

    lax.fori_loop(0, rows, issue, 0, unroll=8)
    local = ids_row_ref[...] - base
    owned = (local >= 0) & (local < vocab)
    want = lax.broadcasted_iota(jnp.int32, (rows * 8, rows), 1) * 8 + (local & 7)
    here = lax.broadcasted_iota(jnp.int32, (rows * 8, rows), 0)
    pick = jnp.where((here == want) & owned, 1.0, 0.0).astype(BF16)
    pltpu.make_async_copy(emb_ref.at[pl.ds(0, rows * 8), :], buf, sem).wait()
    out_ref[...] = lax.dot_general(pick, buf[...], (((0,), (0,)), ((), ())), preferred_element_type=F32).astype(BF16)


def main_kernel(n, hidden_ref, emb_ref, h_gain, e_gain, f_gain, o_gain,
                proj_hbm, gate_hbm, up_hbm, down_hbm, head_hbm,
                z_ref, lse_ref, u_ref,
                proj_v, gate_v, up_v, down_v, ring, emb_in, emb_mine, emb_all, p_mine, p_all,
                part_v, part_in, u_mine, u_all, o_v, stat_mine, stat_in, f_wide, o_wide, m_v, s_v,
                w_sem, ring_sem, send_sem, recv_sem):
    me = lax.axis_index("tp")
    rows, dim = hidden_ref.shape
    chunk = rows // n
    cols = p_mine.shape[0]
    vocab = head_hbm.shape[0]
    tiles = vocab // TILE
    rest = vocab - tiles * TILE

    weights = [pltpu.make_async_copy(src, dst, w_sem.at[i]) for i, (src, dst) in enumerate(
        ((proj_hbm, proj_v), (gate_hbm, gate_v), (up_hbm, up_v), (down_hbm, down_v)))]
    for copy in weights:
        copy.start()

    def head_copy(t):
        slot = lax.rem(t, SLOTS)
        start = pl.multiple_of(t * TILE, TILE)
        return pltpu.make_async_copy(head_hbm.at[pl.ds(start, TILE), :], ring.at[slot], ring_sem.at[slot])

    barrier = pltpu.get_barrier_semaphore()
    for d in range(1, n):
        pl.semaphore_signal(barrier, inc=1, device_id={"tp": lax.rem(me + d, n)}, device_id_type=MESH)
    pl.semaphore_wait(barrier, n - 1)

    def exchange(phase, source, target):
        copies = []
        for d in range(1, n):
            peer = lax.rem(me + d, n)
            copies.append(pltpu.make_async_remote_copy(
                src_ref=source(peer), dst_ref=target(d), send_sem=send_sem.at[phase, d - 1],
                recv_sem=recv_sem.at[phase, d - 1], device_id={"tp": peer}, device_id_type=MESH))
        for copy in copies:
            copy.start()
        return copies

    def part(ref, j, size):
        return ref.at[pl.ds(pl.multiple_of(j * size, size), size), :]

    first = exchange(0, lambda j: part(emb_ref, j, chunk), lambda d: emb_in.at[d - 1])

    def prefetch(t, carry):
        head_copy(t).start()
        return carry

    lax.fori_loop(0, SLOTS, prefetch, 0)

    normed_h = rms(hidden_ref[...], h_gain[...], -1).astype(BF16)
    weights[0].wait()
    acc_h = dot_t(proj_v[:, :dim], normed_h)
    f_wide[...] = jnp.transpose(jnp.broadcast_to(f_gain[...], (rows, dim)))
    o_wide[...] = jnp.transpose(jnp.broadcast_to(o_gain[...], (rows, dim)))
    total = part(emb_ref, me, chunk)[...].astype(F32)
    for d in range(1, n):
        first[d - 1].wait_recv()
        total = total + emb_in[d - 1].astype(F32)
    emb_mine[...] = rms(total, e_gain[...], -1).astype(BF16)
    second = exchange(1, lambda j: emb_mine, lambda d: part(emb_all, me, chunk))
    part(emb_all, me, chunk)[...] = emb_mine[...]
    for copy in second:
        copy.wait_recv()
    p_mine[...] = (acc_h + dot_t(proj_v[:, dim:], emb_all[...])).astype(BF16)

    third = exchange(2, lambda j: p_mine, lambda d: part(p_all, me, cols))
    part(p_all, me, cols)[...] = p_mine[...]
    for copy in third:
        copy.wait_recv()
    normed = rms(p_all[...], f_wide[...], 0).astype(BF16)
    weights[1].wait()
    gate = jnp.dot(gate_v[...], normed, preferred_element_type=F32)
    weights[2].wait()
    up = jnp.dot(up_v[...], normed, preferred_element_type=F32)
    act = (jax.nn.silu(gate) * up).astype(BF16)
    weights[3].wait()
    down = lax.dot_general(act, down_v[...], (((0,), (0,)), ((), ())), preferred_element_type=F32)
    part_v[...] = jnp.transpose(down)

    fourth = exchange(3, lambda j: part(part_v, j, cols), lambda d: part_in.at[d - 1])
    total = part(part_v, me, cols)[...]
    for d in range(1, n):
        fourth[d - 1].wait_recv()
        total = total + part_in[d - 1]
    u_mine[...] = (p_mine[...].astype(F32) + total).astype(BF16)
    fifth = exchange(4, lambda j: u_mine, lambda d: part(u_all, me, cols))
    part(u_all, me, cols)[...] = u_mine[...]
    for copy in fifth:
        copy.wait_recv()
    o_v[...] = rms(u_all[...], o_wide[...], 0).astype(BF16)
    u_ref[...] = u_all[...]

    m_v[...] = jnp.full_like(m_v, -jnp.inf)
    s_v[...] = jnp.zeros_like(s_v)

    def fold(block):
        groups = block.reshape(block.shape[0] // 8, 8, rows)
        old = m_v[...]
        new = jnp.maximum(old, jnp.max(groups, axis=0))
        s_v[...] = s_v[...] * jnp.exp(old - new) + jnp.sum(jnp.exp(groups - new[None]), axis=0)
        m_v[...] = new

    def tile(t, carry):
        head_copy(t).wait()
        block = jnp.dot(ring[lax.rem(t, SLOTS)], o_v[...], preferred_element_type=F32)
        z_ref[pl.ds(pl.multiple_of(t * TILE, TILE), TILE), :] = block
        fold(block)

        @pl.when(t + SLOTS < tiles)
        def _():
            head_copy(t + SLOTS).start()

        @pl.when(t + SLOTS == tiles)
        def _():
            tail_copy().start()
        return carry

    def tail_copy():
        slot = tiles % SLOTS
        return pltpu.make_async_copy(head_hbm.at[pl.ds(tiles * TILE, rest), :], ring.at[slot, pl.ds(0, rest), :], ring_sem.at[slot])

    lax.fori_loop(0, tiles, tile, 0)
    tail_copy().wait()
    block = jnp.dot(ring[tiles % SLOTS, :rest, :], o_v[...], preferred_element_type=F32)
    z_ref[tiles * TILE:, :] = block
    fold(block)

    m_row = jnp.max(m_v[...], axis=0, keepdims=True)
    s_row = jnp.sum(s_v[...] * jnp.exp(m_v[...] - m_row), axis=0, keepdims=True)
    stat_mine[...] = jnp.concatenate([m_row, s_row, jnp.zeros((6, rows), F32)], axis=0)
    sixth = exchange(5, lambda j: stat_mine, lambda d: stat_in.at[me])
    stat_in[me] = stat_mine[...]
    for copy in sixth:
        copy.wait_recv()
    stats = stat_in[...]
    m_all, s_all = stats[:, 0, :], stats[:, 1, :]
    m_top = jnp.max(m_all, axis=0, keepdims=True)
    lse = m_top + jnp.log(jnp.sum(s_all * jnp.exp(m_all - m_top), axis=0, keepdims=True))
    lse_ref[...] = jnp.broadcast_to(lse, lse_ref.shape)
    for group in (first, second, third, fourth, fifth, sixth):
        for copy in group:
            copy.wait_send()


def close_kernel(z_ref, lse_ref, u_in, out_ref, u_out):
    depth, vocab = out_ref.shape[0], z_ref.shape[0]
    i, full = pl.program_id(0), vocab // depth
    rest = vocab - full * depth

    @pl.when(i < full)
    def _():
        out_ref[...] = z_ref[pl.ds(pl.multiple_of(i * depth, depth), depth), :] - lse_ref[0:1, :]

    @pl.when(i == full)
    def _():
        out_ref[:rest, :] = z_ref[full * depth:, :] - lse_ref[0:1, :]

    @pl.when(i == 0)
    def _():
        u_out[...] = jnp.transpose(u_in[...])


def solution(mesh):
    n = mesh.shape["tp"]

    def draft_step(hidden, tokens, embedding, head_w, h_norm, e_norm, f_norm, o_norm, proj_w, w_gate, w_up, w_down):
        rows, dim = hidden.shape
        vocab = head_w.shape[1]
        cols, ffn = proj_w.shape[1], w_gate.shape[1]
        chunk = rows // n
        smem = pl.BlockSpec(memory_space=pltpu.SMEM)
        vmem = pl.BlockSpec(memory_space=pltpu.VMEM)
        hbm = pl.BlockSpec(memory_space=pl.ANY)
        emb_rows = pl.pallas_call(
            gather_kernel,
            out_shape=jax.ShapeDtypeStruct((rows, dim), BF16),
            in_specs=[smem, vmem, hbm],
            out_specs=vmem,
            scratch_shapes=[pltpu.VMEM((rows * 8, dim), BF16), pltpu.SemaphoreType.DMA],
            name="gather_rows",
        )(tokens, tokens[None, :], embedding)

        dma, sem2 = pltpu.SemaphoreType.DMA, (6, n - 1)
        z, lse, u = pl.pallas_call(
            functools.partial(main_kernel, n),
            out_shape=(pltpu.VMEM((vocab, rows), F32), pltpu.VMEM((8, rows), F32), pltpu.VMEM((dim, rows), BF16)),
            in_specs=[vmem] * 6 + [hbm] * 5,
            out_specs=(vmem, vmem, vmem),
            scratch_shapes=[
                pltpu.VMEM((cols, 2 * dim), BF16), pltpu.VMEM((ffn, dim), BF16), pltpu.VMEM((ffn, dim), BF16),
                pltpu.VMEM((ffn, dim), BF16), pltpu.VMEM((SLOTS, TILE, dim), BF16),
                pltpu.VMEM((n - 1, chunk, dim), BF16), pltpu.VMEM((chunk, dim), BF16), pltpu.VMEM((rows, dim), BF16),
                pltpu.VMEM((cols, rows), BF16), pltpu.VMEM((dim, rows), BF16),
                pltpu.VMEM((dim, rows), F32), pltpu.VMEM((n - 1, cols, rows), F32),
                pltpu.VMEM((cols, rows), BF16), pltpu.VMEM((dim, rows), BF16), pltpu.VMEM((dim, rows), BF16),
                pltpu.VMEM((8, rows), F32), pltpu.VMEM((n, 8, rows), F32),
                pltpu.VMEM((dim, rows), F32), pltpu.VMEM((dim, rows), F32),
                pltpu.VMEM((8, rows), F32), pltpu.VMEM((8, rows), F32),
                dma((4,)), dma((SLOTS,)), dma(sem2), dma(sem2),
            ],
            compiler_params=pltpu.CompilerParams(
                collective_id=0, has_side_effects=True, vmem_limit_bytes=53 * 1024 * 1024),
            name="draft_main",
        )(hidden, emb_rows, h_norm[None], e_norm[None], f_norm[None], o_norm[None],
          proj_w.T, w_gate.T, w_up.T, w_down, head_w.T)

        depth = 1920
        logp, new_u = pl.pallas_call(
            close_kernel,
            grid=(pl.cdiv(vocab, depth),),
            out_shape=(jax.ShapeDtypeStruct((vocab, rows), F32), jax.ShapeDtypeStruct((rows, dim), BF16)),
            in_specs=[vmem, vmem, vmem],
            out_specs=(pl.BlockSpec((depth, rows), lambda i: (i, 0)), pl.BlockSpec((rows, dim), lambda i: (0, 0))),
            compiler_params=pltpu.CompilerParams(vmem_limit_bytes=16 * 1024 * 1024),
            name="close",
        )(z, lse, u)
        return new_u, logp.T

    specs_in = (P("dp", None), P("dp"), P("tp", None), P(None, "tp"), P(None), P(None), P(None), P(None), P(None, "tp"), P(None, "tp"), P(None, "tp"), P("tp", None))
    specs_out = (P("dp", None), P("dp", "tp"))
    return jax.shard_map(draft_step, mesh=mesh, in_specs=specs_in, out_specs=specs_out, check_vma=False)
```

```python
import functools

import jax
import jax.numpy as jnp
from jax import lax
from jax.experimental import pallas as pl
from jax.experimental.pallas import tpu as pltpu
from jax.sharding import PartitionSpec as P

NORM_EPS = 1e-6
BLOCK = 1024
SLOTS = 12
MAIN_MIB = 17
PAIR = 3
HEAD_MIB = 17
CLOSE = 1024
MESH = pl.DeviceIdType.MESH
F32, BF16 = jnp.float32, jnp.bfloat16


def rms(values, gain, axis):
    wide = values.astype(F32)
    inv = lax.rsqrt(jnp.mean(wide * wide, axis=axis, keepdims=True) + NORM_EPS)
    return wide * inv * gain


def dot_t(a, b):
    return lax.dot_general(a, b, (((1,), (1,)), ((), ())), preferred_element_type=F32)


def gather_kernel(ids_ref, ids_row_ref, emb_ref, out_ref, buf, sem):
    rows, vocab = out_ref.shape[0], emb_ref.shape[0]
    base = lax.axis_index("tp") * vocab

    def issue(r, carry):
        local = jnp.clip(ids_ref[r] - base, 0, vocab - 1)
        start = pl.multiple_of((local // 8) * 8, 8)
        pltpu.make_async_copy(emb_ref.at[pl.ds(start, 8), :], buf.at[pl.ds(pl.multiple_of(r * 8, 8), 8), :], sem).start()
        return carry

    lax.fori_loop(0, rows, issue, 0, unroll=8)
    local = ids_row_ref[...] - base
    owned = (local >= 0) & (local < vocab)
    want = lax.broadcasted_iota(jnp.int32, (rows * 8, rows), 1) * 8 + (local & 7)
    here = lax.broadcasted_iota(jnp.int32, (rows * 8, rows), 0)
    pick = jnp.where((here == want) & owned, 1.0, 0.0).astype(BF16)
    pltpu.make_async_copy(emb_ref.at[pl.ds(0, rows * 8), :], buf, sem).wait()
    out_ref[...] = lax.dot_general(pick, buf[...], (((0,), (0,)), ((), ())), preferred_element_type=F32).astype(BF16)


def main_kernel(n, hidden_ref, emb_ref, h_gain, e_gain, f_gain, o_gain,
                proj_hbm, gate_hbm, up_hbm, down_hbm, head_hbm,
                ring, o_v, o_rows, u_ref,
                proj_v, gate_v, up_v, down_v, emb_pair, emb_sum, emb_in, emb_mine, emb_all, p_mine, p_all,
                part_v, pair_in, sum_v, part_in, u_mine, u_all, f_wide, o_wide,
                w_sem, ring_sem, send_sem, recv_sem):
    me = lax.axis_index("tp")
    rows, dim = hidden_ref.shape
    chunk, half = rows // n, rows // 2
    cols = p_mine.shape[0]

    core, chip = lax.rem(me, 2), lax.div(me, 2)
    partner = me + 1 - 2 * core
    x, y = lax.rem(chip, 2), lax.div(chip, 2)
    chips = (chip, chip + 1 - 2 * x, chip + 2 - 4 * y, 3 - chip)
    far = (3, 1, 2)

    weights = [pltpu.make_async_copy(src, dst, w_sem.at[i]) for i, (src, dst) in enumerate(
        ((proj_hbm, proj_v), (gate_hbm, gate_v), (up_hbm, up_v), (down_hbm, down_v)))]
    for copy in weights:
        copy.start()

    def head_copy(t):
        at = pl.ds(pl.multiple_of(t * BLOCK, BLOCK), BLOCK)
        return pltpu.make_async_copy(head_hbm.at[at, :], ring.at[at, :], ring_sem.at[t])

    barrier = pltpu.get_barrier_semaphore()
    for d in range(1, n):
        pl.semaphore_signal(barrier, inc=1, device_id={"tp": lax.rem(me + d, n)}, device_id_type=MESH)
    normed_h = rms(hidden_ref[...], h_gain[...][None, :], -1).astype(BF16)
    pl.semaphore_wait(barrier, n - 1)

    sent = []

    def send(source, target, device):
        i = len(sent)
        copy = pltpu.make_async_remote_copy(src_ref=source, dst_ref=target, send_sem=send_sem.at[i], recv_sem=recv_sem.at[i],
                                            device_id={"tp": device}, device_id_type=MESH)
        copy.start()
        sent.append(copy)
        return copy

    def part(ref, j, size):
        return ref.at[pl.ds(pl.multiple_of(j * size, size), size), :]

    def all_gather(mine, place):
        arriving = {m: send(mine, place(me), chips[m] * 2 + core) for m in far}
        beside = [send(mine, place(me), partner)]
        place(me)[...] = mine[...]
        for m in (1, 2, 3):
            arriving[m].wait_recv()
            there = place(chips[m] * 2 + core)
            beside.append(send(there, there, partner))
        for copy in beside:
            copy.wait_recv()

    pair = send(part(emb_ref, 1 - core, half), emb_pair, partner)

    def prefetch(t, carry):
        head_copy(t).start()
        return carry

    lax.fori_loop(0, SLOTS, prefetch, 0)
    pair.wait_recv()
    emb_sum[...] = part(emb_ref, core, half)[...] + emb_pair[...]
    first = [send(part(emb_sum, chips[m], chunk), emb_in.at[m - 1], chips[m] * 2 + core) for m in far]
    weights[0].wait()
    acc_h = dot_t(proj_v[:, :dim], normed_h)
    total = part(emb_sum, chip, chunk)[...].astype(F32)
    for copy in first:
        copy.wait_recv()
    for m in (0, 1, 2):
        total = total + emb_in[m].astype(F32)
    emb_mine[...] = rms(total, e_gain[...][None, :], -1).astype(BF16)
    all_gather(emb_mine, lambda j: part(emb_all, lax.rem(j, 2) * (n // 2) + lax.div(j, 2), chunk))
    p_mine[...] = (acc_h + dot_t(proj_v[:, dim:], emb_all[...])).astype(BF16)

    all_gather(p_mine, lambda j: part(p_all, j, cols))
    f_wide[...] = jnp.transpose(jnp.broadcast_to(f_gain[...][None, :], (rows, dim)))
    normed = rms(p_all[...], f_wide[...], 0).astype(BF16)
    weights[1].wait()
    gate = jnp.dot(gate_v[...], normed, preferred_element_type=F32)
    weights[2].wait()
    up = jnp.dot(up_v[...], normed, preferred_element_type=F32)
    act = jnp.transpose((jax.nn.silu(gate) * up).astype(BF16))
    weights[3].wait()

    pairs = {}
    for m in (3, 1, 2, 0):
        block = jnp.dot(act, down_v[:, pl.ds(pl.multiple_of(chips[m] * 2 * cols, 2 * cols), 2 * cols)], preferred_element_type=F32)
        part_v[m] = jnp.transpose(block)
        pairs[m] = send(part_v.at[m, pl.ds(pl.multiple_of((1 - core) * cols, cols), cols), :], pair_in.at[m], partner)
    mine = pl.ds(pl.multiple_of(core * cols, cols), cols)
    arriving = []
    for m in far:
        pairs[m].wait_recv()
        sum_v[m - 1] = part_v[m, mine, :] + pair_in[m]
        arriving.append(send(sum_v.at[m - 1], part_in.at[m - 1], chips[m] * 2 + core))
    pairs[0].wait_recv()
    total = part_v[0, mine, :] + pair_in[0]
    for copy in arriving:
        copy.wait_recv()
    for m in (0, 1, 2):
        total = total + part_in[m]
    u_mine[...] = (p_mine[...].astype(F32) + total).astype(BF16)
    o_wide[...] = jnp.transpose(jnp.broadcast_to(o_gain[...][None, :], (rows, dim)))
    all_gather(u_mine, lambda j: part(u_all, j, cols))
    normed_o = rms(u_all[...], o_wide[...], 0).astype(BF16)
    o_v[:, :rows] = normed_o
    o_v[:, rows:] = jnp.zeros_like(normed_o)
    o_rows[...] = jnp.transpose(normed_o)
    u_ref[...] = u_all[...]

    def drain(t, carry):
        head_copy(t).wait()
        return carry

    lax.fori_loop(0, SLOTS, drain, 0)
    for copy in sent:
        copy.wait_send()


def head_kernel(ring, o_v, o_rows, head_hbm, z_ref, stat_ref, stream, end_v, m_v, s_v, stream_sem):
    rows, dim = o_rows.shape
    vocab = head_hbm.shape[0]
    blocks = vocab // BLOCK
    rest = vocab - blocks * BLOCK
    pair = stream.shape[0]
    trips = (blocks - SLOTS) // pair
    held = SLOTS // trips

    def stream_copy(t, b):
        at = pl.multiple_of((SLOTS + t * pair + b) * BLOCK, BLOCK)
        return pltpu.make_async_copy(head_hbm.at[pl.ds(at, BLOCK), :], stream.at[b], stream_sem.at[b])

    end_copy = pltpu.make_async_copy(head_hbm.at[pl.ds(blocks * BLOCK, rest), :], end_v, stream_sem.at[pair])
    for b in range(pair):
        stream_copy(0, b).start()
    end_copy.start()

    m_v[...] = jnp.full_like(m_v, -jnp.inf)
    s_v[...] = jnp.zeros_like(s_v)

    def fold(block):
        groups = block.reshape(block.shape[0] // 8, 8, rows)
        old = m_v[...]
        new = jnp.maximum(old, jnp.max(groups, axis=0))
        s_v[...] = s_v[...] * jnp.exp(old - new) + jnp.sum(jnp.exp(groups - new[None]), axis=0)
        m_v[...] = new

    def head(*accs):
        def trip(i, carry):
            steps = [(b, k) for b in range(held + pair) for k in range(dim // 256)]

            def weights(b, at, k):
                lanes = slice(k * 256, (k + 1) * 256)
                if b < held:
                    return ring[pl.ds(pl.multiple_of((i * held + b) * BLOCK + at, 256), 256), lanes]
                return stream[b - held, at:at + 256, lanes]

            def push_w(j):
                b, k = steps[j]
                if b >= held and k == 0:
                    stream_copy(i, b - held).wait()
                for q in (0, 1):
                    pltpu.matmul_push_rhs(weights(b, q * 512, k), staging_register=0, mxu_index=q, transpose=True)

            def push_o(j):
                k = steps[j][1]
                for q in (0, 1):
                    pltpu.matmul_push_rhs(o_v[k * 256:(k + 1) * 256, :], staging_register=1, mxu_index=q, transpose=False)

            def pops(b):
                block = i * held + b if b < held else SLOTS + i * pair + b - held
                at = pl.multiple_of(block * BLOCK, BLOCK)
                for q in (0, 1):
                    block = jnp.transpose(pltpu.matmul_pop(accs[q * 4 + b % 2 * 2]))
                    z_ref[pl.ds(at + q * 512, 256), :] = block
                    fold(block)
                    block = pltpu.matmul_pop(accs[q * 4 + b % 2 * 2 + 1])[:, :rows]
                    z_ref[pl.ds(at + q * 512 + 256, 256), :] = block
                    fold(block)

            push_w(0)
            push_o(0)
            for j, (b, k) in enumerate(steps):
                for q in (0, 1):
                    pltpu.matmul_acc_lhs(accs[q * 4 + b % 2 * 2], o_rows[:, k * 256:(k + 1) * 256], load_staged_rhs=0)
                if j + 1 < len(steps):
                    push_w(j + 1)
                for q in (0, 1):
                    pltpu.matmul_acc_lhs(accs[q * 4 + b % 2 * 2 + 1], weights(b, q * 512 + 256, k), load_staged_rhs=1)
                if j + 1 < len(steps):
                    push_o(j + 1)
                if k == 2 and b > 0:
                    pops(b - 1)
            pops(held + pair - 1)

            @pl.when(i + 1 < trips)
            def _():
                for b in range(pair):
                    stream_copy(i + 1, b).start()
            return carry

        lax.fori_loop(0, trips, trip, 0)

    pl.run_scoped(head, *[pltpu.ACC(q)((size, 256), F32) for q in (0, 1) for _ in (0, 1) for size in (128, 256)])
    end_copy.wait()
    first_rows = rest // 32 * 16
    sizes = (first_rows, rest - first_rows)

    def tail(*accs):
        for k in range(dim // 256):
            for q in (0, 1):
                pltpu.matmul_push_rhs(o_v[k * 256:(k + 1) * 256, :], staging_register=k % 2, mxu_index=q, transpose=False)
                pltpu.matmul_acc_lhs(accs[q], end_v[q * sizes[0]:q * sizes[0] + sizes[q], k * 256:(k + 1) * 256], load_staged_rhs=k % 2)
        for q in (0, 1):
            block = pltpu.matmul_pop(accs[q])[:, :rows]
            z_ref[pl.ds(blocks * BLOCK + q * sizes[0], sizes[q]), :] = block
            fold(block)

    pl.run_scoped(tail, *[pltpu.ACC(q)((sizes[q], 256), F32) for q in (0, 1)])
    m_row = jnp.max(m_v[...], axis=0, keepdims=True)
    s_row = jnp.sum(s_v[...] * jnp.exp(m_v[...] - m_row), axis=0, keepdims=True)
    stat_ref[...] = jnp.concatenate([m_row, s_row, jnp.zeros((6, rows), F32)], axis=0)


def total_kernel(n, stat_ref, lse_ref, stat_in, send_sem, recv_sem):
    me = lax.axis_index("tp")
    barrier = pltpu.get_barrier_semaphore()
    for d in range(1, n):
        pl.semaphore_signal(barrier, inc=1, device_id={"tp": lax.rem(me + d, n)}, device_id_type=MESH)
    stat_in[me] = stat_ref[...]
    pl.semaphore_wait(barrier, n - 1)
    copies = []
    for d in (4, 6, 2, 3, 5, 7, 1):
        copies.append(pltpu.make_async_remote_copy(
            src_ref=stat_ref, dst_ref=stat_in.at[me], send_sem=send_sem.at[d - 1], recv_sem=recv_sem.at[d - 1],
            device_id={"tp": lax.rem(me + d, n)}, device_id_type=MESH))
        copies[-1].start()
    for copy in copies:
        copy.wait_recv()
    stats = stat_in[...]
    m_all, s_all = stats[:, 0, :], stats[:, 1, :]
    m_top = jnp.max(m_all, axis=0, keepdims=True)
    lse = m_top + jnp.log(jnp.sum(s_all * jnp.exp(m_all - m_top), axis=0, keepdims=True))
    lse_ref[...] = jnp.broadcast_to(lse, lse_ref.shape)
    for copy in copies:
        copy.wait_send()


def close_kernel(z_ref, lse_ref, u_in, logp_hbm, u_hbm, stage, u_stage, sem):
    vocab = z_ref.shape[0]
    copies = []
    for i, at in enumerate(range(0, vocab, CLOSE)):
        size = min(CLOSE, vocab - at)
        stage[at:at + size, :] = z_ref[at:at + size, :] - lse_ref[0:1, :]
        copies.append(pltpu.make_async_copy(stage.at[pl.ds(at, size), :], logp_hbm.at[pl.ds(at, size), :], sem.at[i]))
        copies[-1].start()
    u_stage[...] = jnp.transpose(u_in[...])
    copies.append(pltpu.make_async_copy(u_stage, u_hbm, sem.at[len(copies)]))
    copies[-1].start()
    for copy in copies:
        copy.wait()


def solution(mesh):
    n = mesh.shape["tp"]

    def draft_step(hidden, tokens, embedding, head_w, h_norm, e_norm, f_norm, o_norm, proj_w, w_gate, w_up, w_down):
        rows, dim = hidden.shape
        vocab = head_w.shape[1]
        cols, ffn = proj_w.shape[1], w_gate.shape[1]
        chunk = rows // n
        smem = pl.BlockSpec(memory_space=pltpu.SMEM)
        vmem = pl.BlockSpec(memory_space=pltpu.VMEM)
        hbm = pl.BlockSpec(memory_space=pl.ANY)
        emb_rows = pl.pallas_call(
            gather_kernel,
            out_shape=jax.ShapeDtypeStruct((rows, dim), BF16),
            in_specs=[smem, vmem, hbm],
            out_specs=vmem,
            scratch_shapes=[pltpu.VMEM((rows * 8, dim), BF16), pltpu.SemaphoreType.DMA],
            name="gather_rows",
        )(tokens, tokens[None, :], embedding)

        dma = pltpu.SemaphoreType.DMA
        head_t = head_w.T
        ring, o_pad, o_rows, u = pl.pallas_call(
            functools.partial(main_kernel, n),
            out_shape=(pltpu.VMEM((SLOTS * BLOCK, dim), BF16), pltpu.VMEM((dim, 2 * rows), BF16), pltpu.VMEM((rows, dim), BF16),
                       pltpu.VMEM((dim, rows), BF16)),
            in_specs=[vmem] * 6 + [hbm] * 5,
            out_specs=(vmem, vmem, vmem, vmem),
            scratch_shapes=[
                pltpu.VMEM((cols, 2 * dim), BF16), pltpu.VMEM((ffn, dim), BF16), pltpu.VMEM((ffn, dim), BF16),
                pltpu.VMEM((ffn, dim), BF16),
                pltpu.VMEM((rows // 2, dim), BF16), pltpu.VMEM((rows // 2, dim), BF16), pltpu.VMEM((3, chunk, dim), BF16),
                pltpu.VMEM((chunk, dim), BF16), pltpu.VMEM((rows, dim), BF16),
                pltpu.VMEM((cols, rows), BF16), pltpu.VMEM((dim, rows), BF16),
                pltpu.VMEM((4, 2 * cols, rows), F32), pltpu.VMEM((4, cols, rows), F32), pltpu.VMEM((3, cols, rows), F32),
                pltpu.VMEM((3, cols, rows), F32),
                pltpu.VMEM((cols, rows), BF16), pltpu.VMEM((dim, rows), BF16),
                pltpu.VMEM((dim, rows), F32), pltpu.VMEM((dim, rows), F32),
                dma((4,)), dma((SLOTS,)), dma((40,)), dma((40,)),
            ],
            compiler_params=pltpu.CompilerParams(
                collective_id=0, has_side_effects=True, vmem_limit_bytes=int(MAIN_MIB * 1024 * 1024)),
            name="draft_main",
        )(hidden, emb_rows, h_norm, e_norm, f_norm, o_norm,
          proj_w.T, w_gate.T, w_up.T, w_down, head_t)

        z, stat = pl.pallas_call(
            head_kernel,
            out_shape=(pltpu.VMEM((vocab, rows), F32), pltpu.VMEM((8, rows), F32)),
            in_specs=[vmem, vmem, vmem, hbm],
            out_specs=(vmem, vmem),
            scratch_shapes=[
                pltpu.VMEM((PAIR, BLOCK, dim), BF16), pltpu.VMEM((vocab % BLOCK, dim), BF16),
                pltpu.VMEM((8, rows), F32), pltpu.VMEM((8, rows), F32), dma((PAIR + 1,))],
            compiler_params=pltpu.CompilerParams(vmem_limit_bytes=int(HEAD_MIB * 1024 * 1024)),
            name="head",
        )(*(pltpu.with_memory_space_constraint(v, pltpu.VMEM) for v in (ring, o_pad, o_rows)), head_t)

        lse = pl.pallas_call(
            functools.partial(total_kernel, n),
            out_shape=pltpu.VMEM((8, rows), F32),
            in_specs=[vmem],
            out_specs=vmem,
            scratch_shapes=[pltpu.VMEM((n, 8, rows), F32), dma((n - 1,)), dma((n - 1,))],
            compiler_params=pltpu.CompilerParams(collective_id=1, has_side_effects=True, vmem_limit_bytes=4 * 1024 * 1024),
            name="total",
        )(stat)

        logp, new_u = pl.pallas_call(
            close_kernel,
            out_shape=(jax.ShapeDtypeStruct((vocab, rows), F32), jax.ShapeDtypeStruct((rows, dim), BF16)),
            in_specs=[vmem, vmem, vmem],
            out_specs=(hbm, hbm),
            scratch_shapes=[pltpu.VMEM((vocab, rows), F32), pltpu.VMEM((rows, dim), BF16), dma((pl.cdiv(vocab, CLOSE) + 1,))],
            compiler_params=pltpu.CompilerParams(vmem_limit_bytes=16 * 1024 * 1024),
            name="close",
        )(z, lse, u)
        return new_u, logp.T

    specs_in = (P("dp", None), P("dp"), P("tp", None), P(None, "tp"), P(None), P(None), P(None), P(None), P(None, "tp"), P(None, "tp"), P(None, "tp"), P("tp", None))
    specs_out = (P("dp", None), P("dp", "tp"))
    return jax.shard_map(draft_step, mesh=mesh, in_specs=specs_in, out_specs=specs_out, check_vma=False)
```

```python
import functools

import jax
import jax.numpy as jnp
from jax import lax
from jax.experimental import pallas as pl
from jax.experimental.pallas import tpu as pltpu
from jax.sharding import PartitionSpec as P

NORM_EPS = 1e-6
BLOCK = 1024
SLOTS = 10
MAIN_MIB = 23.4
PAIR = 4
HEAD_MIB = 23.4
GATHER_MIB = 60
CLOSE = 1024
MESH = pl.DeviceIdType.MESH
F32, BF16 = jnp.float32, jnp.bfloat16


def rms(values, gain, axis):
    wide = values.astype(F32)
    inv = lax.rsqrt(jnp.mean(wide * wide, axis=axis, keepdims=True) + NORM_EPS)
    return wide * inv * gain


def dot_t(a, b):
    return lax.dot_general(a, b, (((1,), (1,)), ((), ())), preferred_element_type=F32)


def gather_kernel(ids_ref, ids_row_ref, emb_hbm, hidden_hbm, h_gain, e_gain, emb_ref, hid_ref, buf, hid_v, sem):
    rows, dim = emb_ref.shape
    vocab = emb_hbm.shape[0]
    base = lax.axis_index("tp") * vocab

    def issue(r, carry):
        local = ids_ref[r] - base
        local = jnp.where((local >= 0) & (local < vocab), local, r * 8)
        start = pl.multiple_of((local // 8) * 8, 8)
        pltpu.make_async_copy(emb_hbm.at[pl.ds(start, 8), :], buf.at[pl.ds(pl.multiple_of(r * 8, 8), 8), :], sem.at[0]).start()
        return carry

    lax.fori_loop(0, rows, issue, 0, unroll=16)
    hid_copy = pltpu.make_async_copy(hidden_hbm, hid_v, sem.at[1])
    hid_copy.start()
    local = ids_row_ref[...] - base
    owned = (local >= 0) & (local < vocab)
    want = lax.broadcasted_iota(jnp.int32, (rows * 8, rows), 1) * 8 + (local & 7)
    here = lax.broadcasted_iota(jnp.int32, (rows * 8, rows), 0)
    pick = jnp.where((here == want) & owned, 1.0, 0.0).astype(BF16)
    hid_copy.wait()
    hid_ref[...] = rms(hid_v[...], h_gain[...][None, :], -1).astype(BF16)
    pltpu.make_async_copy(emb_hbm.at[pl.ds(0, rows * 8), :], buf, sem.at[0]).wait()
    picked = lax.dot_general(pick, buf[...], (((0,), (0,)), ((), ())), preferred_element_type=F32)
    emb_ref[...] = rms(picked, e_gain[...][None, :], -1).astype(BF16)


def main_kernel(n, emb_hbm, hid_hbm, f_gain, o_gain,
                proj_hbm, gate_hbm, up_hbm, down_hbm, head_hbm,
                ring, o_v, o_rows, u_ref,
                emb_ref, hid_ref, proj_v, gate_v, up_v, wide_w, down_v, emb_pair, emb_in, emb_mine, emb_all, p_mine, p_all,
                part_v, pair_in, part_in, u_mine, u_all, wide,
                w_sem, ring_sem, send_sem, recv_sem):
    me = lax.axis_index("tp")
    rows, dim = hid_ref.shape
    chunk, half = rows // n, rows // 2
    cols, ffn = p_mine.shape[0], gate_hbm.shape[0]

    core, chip = lax.rem(me, 2), lax.div(me, 2)
    partner = me + 1 - 2 * core
    x, y = lax.rem(chip, 2), lax.div(chip, 2)
    chips = (chip, chip + 1 - 2 * x, chip + 2 - 4 * y, 3 - chip)
    far = (3, 1, 2)

    local = [pltpu.make_async_copy(src, dst, w_sem.at[4 + i]) for i, (src, dst) in enumerate(((emb_hbm, emb_ref), (hid_hbm, hid_ref)))]
    for copy in local:
        copy.start()
    weights = [pltpu.make_async_copy(src, dst, w_sem.at[i]) for i, (src, dst) in enumerate(
        ((proj_hbm, proj_v), (gate_hbm, gate_v), (up_hbm, up_v), (down_hbm, down_v)))]
    for copy in weights:
        copy.start()

    def head_copy(t):
        at = pl.ds(pl.multiple_of(t * BLOCK, BLOCK), BLOCK)
        return pltpu.make_async_copy(head_hbm.at[at, :], ring.at[at, :], ring_sem.at[t])

    barrier = pltpu.get_barrier_semaphore()
    for d in range(1, n):
        pl.semaphore_signal(barrier, inc=1, device_id={"tp": lax.rem(me + d, n)}, device_id_type=MESH)
    local[0].wait()
    pl.semaphore_wait(barrier, n - 1)

    sent = []

    def send(source, target, device):
        i = len(sent)
        copy = pltpu.make_async_remote_copy(src_ref=source, dst_ref=target, send_sem=send_sem.at[i], recv_sem=recv_sem.at[i],
                                            device_id={"tp": device}, device_id_type=MESH)
        copy.start()
        sent.append(copy)
        return copy

    def part(ref, j, size):
        return ref.at[pl.ds(pl.multiple_of(j * size, size), size), :]

    def all_gather(mine, place, meanwhile=lambda: None):
        arriving = {m: send(mine, place(me), chips[m] * 2 + core) for m in far}
        beside = [send(mine, place(me), partner)]
        place(me)[...] = mine[...]
        meanwhile()
        for m in (1, 2, 3):
            arriving[m].wait_recv()
            there = place(chips[m] * 2 + core)
            beside.append(send(there, there, partner))
        for copy in beside:
            copy.wait_recv()

    pair = send(part(emb_ref, 1 - core, half), emb_pair, partner)

    def prefetch(t, carry):
        head_copy(t).start()
        return carry

    lax.fori_loop(0, SLOTS, prefetch, 0)
    pair.wait_recv()
    emb_sum = part(emb_ref, core, half)
    emb_sum[...] = emb_sum[...] + emb_pair[...]
    first = [send(part(emb_ref, core * (n // 2) + chips[m], chunk), emb_in.at[m - 1], chips[m] * 2 + core) for m in far]
    turned = pl.cdiv(ffn, 128) * 128

    def turn(i):
        weights[1 + i].wait()
        source = (gate_v, up_v)[i]
        for at in range(0, ffn, 256):
            size = min(256, ffn - at)
            wide_w[:, i * turned + at:i * turned + at + size] = jnp.transpose(source[at:at + size, :])

    weights[0].wait()
    local[1].wait()
    acc_h = dot_t(proj_v[:, :dim], hid_ref[...])
    wide[...] = jnp.transpose(jnp.broadcast_to(f_gain[...][None, :], (rows, dim)))
    turn(0)
    total = part(emb_ref, core * (n // 2) + chip, chunk)[...]
    for copy in first:
        copy.wait_recv()
    for m in (0, 1, 2):
        total = total + emb_in[m]
    emb_mine[...] = total
    all_gather(emb_mine, lambda j: part(emb_all, lax.rem(j, 2) * (n // 2) + lax.div(j, 2), chunk), lambda: turn(1))
    p_mine[...] = (acc_h + dot_t(proj_v[:, dim:], emb_all[...])).astype(BF16)

    all_gather(p_mine, lambda j: part(p_all, j, cols))
    normed = rms(p_all[...], wide[...], 0).astype(BF16)
    hidden = jnp.dot(jnp.transpose(normed), wide_w[...], preferred_element_type=F32)
    act = (jax.nn.silu(hidden[:, :ffn]) * hidden[:, turned:turned + ffn]).astype(BF16)
    weights[3].wait()

    pairs = {}
    for m in (3, 1, 2, 0):
        block = jnp.dot(act, down_v[:, pl.ds(pl.multiple_of(chips[m] * 2 * cols, 2 * cols), 2 * cols)], preferred_element_type=F32)
        part_v[m] = jnp.transpose(block)
        pairs[m] = send(part_v.at[m, pl.ds(pl.multiple_of((1 - core) * cols, cols), cols), :], pair_in.at[m], partner)
    mine = pl.ds(pl.multiple_of(core * cols, cols), cols)
    arriving = []
    for m in far:
        pairs[m].wait_recv()
        part_v[m, mine, :] = part_v[m, mine, :] + pair_in[m]
        arriving.append(send(part_v.at[m, mine, :], part_in.at[m - 1], chips[m] * 2 + core))
    pairs[0].wait_recv()
    total = part_v[0, mine, :] + pair_in[0]
    wide[...] = jnp.transpose(jnp.broadcast_to(o_gain[...][None, :], (rows, dim)))
    for copy in arriving:
        copy.wait_recv()
    for m in (0, 1, 2):
        total = total + part_in[m]
    u_mine[...] = (p_mine[...].astype(F32) + total).astype(BF16)
    all_gather(u_mine, lambda j: part(u_all, j, cols))
    normed_o = rms(u_all[...], wide[...], 0).astype(BF16)
    o_v[...] = normed_o
    o_rows[...] = jnp.transpose(normed_o)
    u_ref[...] = u_all[...]

    def drain(t, carry):
        head_copy(t).wait()
        return carry

    lax.fori_loop(0, SLOTS, drain, 0)
    for copy in sent:
        copy.wait_send()


def head_kernel(ring, o_in, o_rows, head_hbm, z_ref, stat_ref, stream, end_v, o_v, m_v, s_v, stream_sem):
    rows, dim = o_rows.shape
    vocab = head_hbm.shape[0]
    blocks = vocab // BLOCK
    rest = vocab - blocks * BLOCK
    pair = stream.shape[0]
    trips = (blocks - SLOTS) // pair
    held = SLOTS // trips

    def stream_copy(t, b):
        at = pl.multiple_of((SLOTS + t * pair + b) * BLOCK, BLOCK)
        return pltpu.make_async_copy(head_hbm.at[pl.ds(at, BLOCK), :], stream.at[b], stream_sem.at[b])

    end_copy = pltpu.make_async_copy(head_hbm.at[pl.ds(blocks * BLOCK, rest), :], end_v, stream_sem.at[pair])
    for b in range(pair):
        stream_copy(0, b).start()
    end_copy.start()
    o_v[:, :rows] = o_in[...]
    o_v[:, rows:] = jnp.zeros_like(o_in[...])

    m_v[...] = jnp.full_like(m_v, -jnp.inf)
    s_v[...] = jnp.zeros_like(s_v)

    def fold(block):
        groups = block.reshape(block.shape[0] // 8, 8, rows)
        old = m_v[...]
        new = jnp.maximum(old, jnp.max(groups, axis=0))
        s_v[...] = s_v[...] * jnp.exp(old - new) + jnp.sum(jnp.exp(groups - new[None]), axis=0)
        m_v[...] = new

    def head(*accs):
        def trip(i, carry):
            steps = [(b, k) for b in range(held + pair) for k in range(dim // 256)]

            def weights(b, at, k):
                lanes = slice(k * 256, (k + 1) * 256)
                if b < held:
                    return ring[pl.ds(pl.multiple_of((i * held + b) * BLOCK + at, 256), 256), lanes]
                return stream[b - held, at:at + 256, lanes]

            def push_w(j):
                b, k = steps[j]
                if b >= held and k == 0:
                    stream_copy(i, b - held).wait()
                for q in (0, 1):
                    pltpu.matmul_push_rhs(weights(b, q * 512, k), staging_register=0, mxu_index=q, transpose=True)

            def push_o(j):
                k = steps[j][1]
                for q in (0, 1):
                    pltpu.matmul_push_rhs(o_v[k * 256:(k + 1) * 256, :], staging_register=1, mxu_index=q, transpose=False)

            def pops(b):
                block = i * held + b if b < held else SLOTS + i * pair + b - held
                at = pl.multiple_of(block * BLOCK, BLOCK)
                for q in (0, 1):
                    block = jnp.transpose(pltpu.matmul_pop(accs[q * 4 + b % 2 * 2]))
                    z_ref[pl.ds(at + q * 512, 256), :] = block
                    fold(block)
                    block = pltpu.matmul_pop(accs[q * 4 + b % 2 * 2 + 1])[:, :rows]
                    z_ref[pl.ds(at + q * 512 + 256, 256), :] = block
                    fold(block)

            push_w(0)
            push_o(0)
            for j, (b, k) in enumerate(steps):
                for q in (0, 1):
                    pltpu.matmul_acc_lhs(accs[q * 4 + b % 2 * 2], o_rows[:, k * 256:(k + 1) * 256], load_staged_rhs=0)
                if j + 1 < len(steps):
                    push_w(j + 1)
                for q in (0, 1):
                    pltpu.matmul_acc_lhs(accs[q * 4 + b % 2 * 2 + 1], weights(b, q * 512 + 256, k), load_staged_rhs=1)
                if j + 1 < len(steps):
                    push_o(j + 1)
                if k == 2 and b > 0:
                    pops(b - 1)
            pops(held + pair - 1)

            @pl.when(i + 1 < trips)
            def _():
                for b in range(pair):
                    stream_copy(i + 1, b).start()
            return carry

        lax.fori_loop(0, trips, trip, 0)

    pl.run_scoped(head, *[pltpu.ACC(q)((size, 256), F32) for q in (0, 1) for _ in (0, 1) for size in (128, 256)])
    end_copy.wait()
    first_rows = rest // 32 * 16
    sizes = (first_rows, rest - first_rows)

    def tail(*accs):
        for k in range(dim // 256):
            for q in (0, 1):
                pltpu.matmul_push_rhs(o_v[k * 256:(k + 1) * 256, :], staging_register=k % 2, mxu_index=q, transpose=False)
                pltpu.matmul_acc_lhs(accs[q], end_v[q * sizes[0]:q * sizes[0] + sizes[q], k * 256:(k + 1) * 256], load_staged_rhs=k % 2)
        for q in (0, 1):
            block = pltpu.matmul_pop(accs[q])[:, :rows]
            z_ref[pl.ds(blocks * BLOCK + q * sizes[0], sizes[q]), :] = block
            fold(block)

    pl.run_scoped(tail, *[pltpu.ACC(q)((sizes[q], 256), F32) for q in (0, 1)])
    m_row = jnp.max(m_v[...], axis=0, keepdims=True)
    s_row = jnp.sum(s_v[...] * jnp.exp(m_v[...] - m_row), axis=0, keepdims=True)
    stat_ref[...] = jnp.concatenate([m_row, s_row, jnp.zeros((6, rows), F32)], axis=0)


def total_kernel(n, stat_ref, lse_ref, stat_in, send_sem, recv_sem):
    me = lax.axis_index("tp")
    barrier = pltpu.get_barrier_semaphore()
    for d in range(1, n):
        pl.semaphore_signal(barrier, inc=1, device_id={"tp": lax.rem(me + d, n)}, device_id_type=MESH)
    stat_in[me] = stat_ref[...]
    pl.semaphore_wait(barrier, n - 1)
    copies = []
    for d in (4, 6, 2, 3, 5, 7, 1):
        copies.append(pltpu.make_async_remote_copy(
            src_ref=stat_ref, dst_ref=stat_in.at[me], send_sem=send_sem.at[d - 1], recv_sem=recv_sem.at[d - 1],
            device_id={"tp": lax.rem(me + d, n)}, device_id_type=MESH))
        copies[-1].start()
    for copy in copies:
        copy.wait_recv()
    stats = stat_in[...]
    m_all, s_all = stats[:, 0, :], stats[:, 1, :]
    m_top = jnp.max(m_all, axis=0, keepdims=True)
    lse = m_top + jnp.log(jnp.sum(s_all * jnp.exp(m_all - m_top), axis=0, keepdims=True))
    lse_ref[...] = jnp.broadcast_to(lse, lse_ref.shape)
    for copy in copies:
        copy.wait_send()


def close_kernel(z_ref, lse_ref, u_in, logp_hbm, u_hbm, stage, u_stage, sem):
    vocab = z_ref.shape[0]
    copies = []
    for i, at in enumerate(range(0, vocab, CLOSE)):
        size = min(CLOSE, vocab - at)
        stage[at:at + size, :] = z_ref[at:at + size, :] - lse_ref[0:1, :]
        copies.append(pltpu.make_async_copy(stage.at[pl.ds(at, size), :], logp_hbm.at[pl.ds(at, size), :], sem.at[i]))
        copies[-1].start()
    u_stage[...] = jnp.transpose(u_in[...])
    copies.append(pltpu.make_async_copy(u_stage, u_hbm, sem.at[len(copies)]))
    copies[-1].start()
    for copy in copies:
        copy.wait()


def solution(mesh):
    n = mesh.shape["tp"]

    def draft_step(hidden, tokens, embedding, head_w, h_norm, e_norm, f_norm, o_norm, proj_w, w_gate, w_up, w_down):
        rows, dim = hidden.shape
        vocab = head_w.shape[1]
        cols, ffn = proj_w.shape[1], w_gate.shape[1]
        chunk = rows // n
        smem = pl.BlockSpec(memory_space=pltpu.SMEM)
        vmem = pl.BlockSpec(memory_space=pltpu.VMEM)
        hbm = pl.BlockSpec(memory_space=pl.ANY)
        dma = pltpu.SemaphoreType.DMA
        on_chip = functools.partial(pltpu.with_memory_space_constraint, memory_space=pltpu.VMEM)
        ready = pl.pallas_call(
            gather_kernel,
            out_shape=(jax.ShapeDtypeStruct((rows, dim), BF16),) * 2,
            in_specs=[smem, vmem, hbm, hbm, vmem, vmem],
            out_specs=(vmem, vmem),
            scratch_shapes=[pltpu.VMEM((rows * 8, dim), BF16), pltpu.VMEM((rows, dim), BF16), dma((2,))],
            compiler_params=pltpu.CompilerParams(vmem_limit_bytes=GATHER_MIB * 1024 * 1024),
            name="gather_rows",
        )(tokens, tokens[None, :], embedding, hidden, h_norm, e_norm)

        head_t = head_w.T
        ring, o_cols, o_rows, u = pl.pallas_call(
            functools.partial(main_kernel, n),
            out_shape=(pltpu.VMEM((SLOTS * BLOCK, dim), BF16), pltpu.VMEM((dim, rows), BF16), pltpu.VMEM((rows, dim), BF16),
                       pltpu.VMEM((dim, rows), BF16)),
            in_specs=[hbm, hbm, vmem, vmem] + [hbm] * 5,
            out_specs=(vmem, vmem, vmem, vmem),
            scratch_shapes=[
                pltpu.VMEM((rows, dim), BF16), pltpu.VMEM((rows, dim), BF16),
                pltpu.VMEM((cols, 2 * dim), BF16), pltpu.VMEM((ffn, dim), BF16), pltpu.VMEM((ffn, dim), BF16),
                pltpu.VMEM((dim, 2 * pl.cdiv(ffn, 128) * 128), BF16),
                pltpu.VMEM((ffn, dim), BF16),
                pltpu.VMEM((rows // 2, dim), BF16), pltpu.VMEM((3, chunk, dim), BF16),
                pltpu.VMEM((chunk, dim), BF16), pltpu.VMEM((rows, dim), BF16),
                pltpu.VMEM((cols, rows), BF16), pltpu.VMEM((dim, rows), BF16),
                pltpu.VMEM((4, 2 * cols, rows), F32), pltpu.VMEM((4, cols, rows), F32),
                pltpu.VMEM((3, cols, rows), F32),
                pltpu.VMEM((cols, rows), BF16), pltpu.VMEM((dim, rows), BF16), pltpu.VMEM((dim, rows), F32),
                dma((6,)), dma((SLOTS,)), dma((40,)), dma((40,)),
            ],
            compiler_params=pltpu.CompilerParams(
                collective_id=0, has_side_effects=True, vmem_limit_bytes=int(MAIN_MIB * 1024 * 1024)),
            name="draft_main",
        )(*ready, f_norm, o_norm, proj_w.T, w_gate.T, w_up.T, w_down, head_t)

        z, stat = pl.pallas_call(
            head_kernel,
            out_shape=(pltpu.VMEM((vocab, rows), F32), pltpu.VMEM((8, rows), F32)),
            in_specs=[vmem, vmem, vmem, hbm],
            out_specs=(vmem, vmem),
            scratch_shapes=[
                pltpu.VMEM((PAIR, BLOCK, dim), BF16), pltpu.VMEM((vocab % BLOCK, dim), BF16), pltpu.VMEM((dim, 2 * rows), BF16),
                pltpu.VMEM((8, rows), F32), pltpu.VMEM((8, rows), F32), dma((PAIR + 1,))],
            compiler_params=pltpu.CompilerParams(vmem_limit_bytes=int(HEAD_MIB * 1024 * 1024)),
            name="head",
        )(*map(on_chip, (ring, o_cols, o_rows)), head_t)

        lse = pl.pallas_call(
            functools.partial(total_kernel, n),
            out_shape=pltpu.VMEM((8, rows), F32),
            in_specs=[vmem],
            out_specs=vmem,
            scratch_shapes=[pltpu.VMEM((n, 8, rows), F32), dma((n - 1,)), dma((n - 1,))],
            compiler_params=pltpu.CompilerParams(collective_id=1, has_side_effects=True, vmem_limit_bytes=4 * 1024 * 1024),
            name="total",
        )(stat)

        logp, new_u = pl.pallas_call(
            close_kernel,
            out_shape=(jax.ShapeDtypeStruct((vocab, rows), F32), jax.ShapeDtypeStruct((rows, dim), BF16)),
            in_specs=[vmem, vmem, vmem],
            out_specs=(hbm, hbm),
            scratch_shapes=[pltpu.VMEM((vocab, rows), F32), pltpu.VMEM((rows, dim), BF16), dma((pl.cdiv(vocab, CLOSE) + 1,))],
            compiler_params=pltpu.CompilerParams(vmem_limit_bytes=16 * 1024 * 1024),
            name="close",
        )(z, lse, u)
        return new_u, logp.T

    specs_in = (P("dp", None), P("dp"), P("tp", None), P(None, "tp"), P(None), P(None), P(None), P(None), P(None, "tp"), P(None, "tp"), P(None, "tp"), P("tp", None))
    specs_out = (P("dp", None), P("dp", "tp"))
    return jax.shard_map(draft_step, mesh=mesh, in_specs=specs_in, out_specs=specs_out, check_vma=False)
```

```python
import functools

import jax
import jax.numpy as jnp
from jax import lax
from jax.experimental import pallas as pl
from jax.experimental.pallas import tpu as pltpu
from jax.sharding import PartitionSpec as P

NORM_EPS = 1e-6
BLOCK = 1024
SLOTS = 10
MAIN_MIB = 23.4
PAIR = 4
HEAD_MIB = 23.4
GATHER_MIB = 60
CLOSE = 1024
MESH = pl.DeviceIdType.MESH
F32, BF16 = jnp.float32, jnp.bfloat16


def rms(values, gain, axis):
    wide = values.astype(F32)
    inv = lax.rsqrt(jnp.mean(wide * wide, axis=axis, keepdims=True) + NORM_EPS)
    return wide * inv * gain


def dot_t(a, b):
    return lax.dot_general(a, b, (((1,), (1,)), ((), ())), preferred_element_type=F32)


def gather_kernel(ids_ref, ids_row_ref, emb_hbm, emb_ref, buf, sem):
    rows = emb_ref.shape[0]
    vocab = emb_hbm.shape[0]
    base = lax.axis_index("tp") * vocab

    def issue(r, carry):
        local = ids_ref[r] - base
        local = jnp.where((local >= 0) & (local < vocab), local, r * 8)
        start = pl.multiple_of((local // 8) * 8, 8)
        pltpu.make_async_copy(emb_hbm.at[pl.ds(start, 8), :], buf.at[pl.ds(pl.multiple_of(r * 8, 8), 8), :], sem).start()
        return carry

    lax.fori_loop(0, rows, issue, 0, unroll=16)
    local = ids_row_ref[...] - base
    owned = (local >= 0) & (local < vocab)
    want = lax.broadcasted_iota(jnp.int32, (rows * 8, rows), 1) * 8 + (local & 7)
    here = lax.broadcasted_iota(jnp.int32, (rows * 8, rows), 0)
    pick = jnp.where((here == want) & owned, 1.0, 0.0).astype(BF16)
    pltpu.make_async_copy(emb_hbm.at[pl.ds(0, rows * 8), :], buf, sem).wait()
    emb_ref[...] = lax.dot_general(pick, buf[...], (((0,), (0,)), ((), ())), preferred_element_type=F32).astype(BF16)


def main_kernel(n, emb_hbm, hid_hbm, h_hbm, e_hbm, f_hbm, o_hbm,
                proj_hbm, gate_hbm, up_hbm, down_hbm, head_hbm,
                ring, o_v, o_rows, u_ref,
                emb_ref, hid_ref, h_gain, e_gain, f_gain, o_gain, proj_v, gate_v, up_v, wide_w, down_v, emb_pair, emb_in, emb_mine, emb_all, p_mine, p_all,
                part_v, pair_in, part_in, u_mine, u_all, wide,
                w_sem, ring_sem, send_sem, recv_sem):
    me = lax.axis_index("tp")
    rows, dim = hid_ref.shape
    chunk, half = rows // n, rows // 2
    cols, ffn = p_mine.shape[0], gate_hbm.shape[0]

    core, chip = lax.rem(me, 2), lax.div(me, 2)
    partner = me + 1 - 2 * core
    x, y = lax.rem(chip, 2), lax.div(chip, 2)
    chips = (chip, chip + 1 - 2 * x, chip + 2 - 4 * y, 3 - chip)
    far = (3, 1, 2)

    local = [pltpu.make_async_copy(src, dst, w_sem.at[4 + i]) for i, (src, dst) in enumerate((
        (emb_hbm, emb_ref), (hid_hbm, hid_ref), (h_hbm, h_gain), (e_hbm, e_gain), (f_hbm, f_gain), (o_hbm, o_gain)))]
    for copy in local:
        copy.start()
    weights = [pltpu.make_async_copy(src, dst, w_sem.at[i]) for i, (src, dst) in enumerate(
        ((proj_hbm, proj_v), (gate_hbm, gate_v), (up_hbm, up_v), (down_hbm, down_v)))]
    for copy in weights:
        copy.start()

    def head_copy(t):
        at = pl.ds(pl.multiple_of(t * BLOCK, BLOCK), BLOCK)
        return pltpu.make_async_copy(head_hbm.at[at, :], ring.at[at, :], ring_sem.at[t])

    barrier = pltpu.get_barrier_semaphore()
    for d in range(1, n):
        pl.semaphore_signal(barrier, inc=1, device_id={"tp": lax.rem(me + d, n)}, device_id_type=MESH)
    local[0].wait()
    pl.semaphore_wait(barrier, n - 1)

    sent = []

    def send(source, target, device):
        i = len(sent)
        copy = pltpu.make_async_remote_copy(src_ref=source, dst_ref=target, send_sem=send_sem.at[i], recv_sem=recv_sem.at[i],
                                            device_id={"tp": device}, device_id_type=MESH)
        copy.start()
        sent.append(copy)
        return copy

    def part(ref, j, size):
        return ref.at[pl.ds(pl.multiple_of(j * size, size), size), :]

    def all_gather(mine, place, meanwhile=lambda: None):
        arriving = {m: send(mine, place(me), chips[m] * 2 + core) for m in far}
        beside = [send(mine, place(me), partner)]
        place(me)[...] = mine[...]
        meanwhile()
        for m in (1, 2, 3):
            arriving[m].wait_recv()
            there = place(chips[m] * 2 + core)
            beside.append(send(there, there, partner))
        for copy in beside:
            copy.wait_recv()

    pair = send(part(emb_ref, 1 - core, half), emb_pair, partner)

    def prefetch(t, carry):
        head_copy(t).start()
        return carry

    lax.fori_loop(0, SLOTS, prefetch, 0)
    for copy in local[1:]:
        copy.wait()
    hid_ref[...] = rms(hid_ref[...], h_gain[...][None, :], -1).astype(BF16)
    pair.wait_recv()
    emb_sum = part(emb_ref, core, half)
    emb_sum[...] = emb_sum[...] + emb_pair[...]
    first = [send(part(emb_ref, core * (n // 2) + chips[m], chunk), emb_in.at[m - 1], chips[m] * 2 + core) for m in far]
    turned = pl.cdiv(ffn, 128) * 128

    def turn(i, begin, end):
        source = (gate_v, up_v)[i]
        for at in range(begin, end, 256):
            size = min(256, end - at)
            wide_w[:, i * turned + at:i * turned + at + size] = jnp.transpose(source[at:at + size, :])

    weights[0].wait()
    acc_h = dot_t(proj_v[:, :dim], hid_ref[...])
    wide[...] = jnp.transpose(jnp.broadcast_to(f_gain[...][None, :], (rows, dim)))
    weights[1].wait()
    turn(0, 0, ffn)
    weights[2].wait()
    total = part(emb_ref, core * (n // 2) + chip, chunk)[...].astype(F32)
    for copy in first:
        copy.wait_recv()
    for m in (0, 1, 2):
        total = total + emb_in[m].astype(F32)
    emb_mine[...] = rms(total, e_gain[...][None, :], -1).astype(BF16)
    all_gather(emb_mine, lambda j: part(emb_all, lax.rem(j, 2) * (n // 2) + lax.div(j, 2), chunk), lambda: turn(1, 0, 512))
    p_mine[...] = (acc_h + dot_t(proj_v[:, dim:], emb_all[...])).astype(BF16)

    all_gather(p_mine, lambda j: part(p_all, j, cols), lambda: turn(1, 512, ffn))
    normed = rms(p_all[...], wide[...], 0).astype(BF16)
    hidden = jnp.dot(jnp.transpose(normed), wide_w[...], preferred_element_type=F32)
    act = (jax.nn.silu(hidden[:, :ffn]) * hidden[:, turned:turned + ffn]).astype(BF16)
    weights[3].wait()

    mine = pl.ds(pl.multiple_of(core * cols, cols), cols)
    other = pl.ds(pl.multiple_of((1 - core) * cols, cols), cols)
    pairs, arriving = {}, []

    def narrow(m):
        columns = pl.ds(pl.multiple_of(chips[m] * 2 * cols, 2 * cols), 2 * cols)
        part_v[m] = jnp.transpose(jnp.dot(act, down_v[:, columns], preferred_element_type=F32))
        pairs[m] = send(part_v.at[m, other, :], pair_in.at[m], partner)

    def pass_on(m):
        pairs[m].wait_recv()
        part_v[m, mine, :] = part_v[m, mine, :] + pair_in[m]
        arriving.append(send(part_v.at[m, mine, :], part_in.at[m - 1], chips[m] * 2 + core))

    narrow(3)
    narrow(1)
    narrow(2)
    pass_on(3)
    pass_on(1)
    narrow(0)
    pass_on(2)
    pairs[0].wait_recv()
    total = part_v[0, mine, :] + pair_in[0]
    wide[...] = jnp.transpose(jnp.broadcast_to(o_gain[...][None, :], (rows, dim)))
    for copy in arriving:
        copy.wait_recv()
    for m in (0, 1, 2):
        total = total + part_in[m]
    u_mine[...] = (p_mine[...].astype(F32) + total).astype(BF16)
    all_gather(u_mine, lambda j: part(u_all, j, cols))
    normed_o = rms(u_all[...], wide[...], 0).astype(BF16)
    o_v[...] = normed_o
    o_rows[...] = jnp.transpose(normed_o)
    u_ref[...] = u_all[...]

    def drain(t, carry):
        head_copy(t).wait()
        return carry

    lax.fori_loop(0, SLOTS, drain, 0)
    for copy in sent:
        copy.wait_send()


def head_kernel(ring, o_in, o_rows, head_hbm, z_ref, stat_ref, stream, end_v, o_v, m_v, s_v, stream_sem):
    rows, dim = o_rows.shape
    vocab = head_hbm.shape[0]
    blocks = vocab // BLOCK
    rest = vocab - blocks * BLOCK
    pair = stream.shape[0]
    trips = (blocks - SLOTS) // pair
    held = SLOTS // trips

    def stream_copy(t, b):
        at = pl.multiple_of((SLOTS + t * pair + b) * BLOCK, BLOCK)
        return pltpu.make_async_copy(head_hbm.at[pl.ds(at, BLOCK), :], stream.at[b], stream_sem.at[b])

    end_copy = pltpu.make_async_copy(head_hbm.at[pl.ds(blocks * BLOCK, rest), :], end_v, stream_sem.at[pair])
    for b in range(pair):
        stream_copy(0, b).start()
    end_copy.start()
    o_v[:, :rows] = o_in[...]
    o_v[:, rows:] = jnp.zeros_like(o_in[...])

    m_v[...] = jnp.full_like(m_v, -jnp.inf)
    s_v[...] = jnp.zeros_like(s_v)

    def fold(block):
        groups = block.reshape(block.shape[0] // 8, 8, rows)
        old = m_v[...]
        new = jnp.maximum(old, jnp.max(groups, axis=0))
        s_v[...] = s_v[...] * jnp.exp(old - new) + jnp.sum(jnp.exp(groups - new[None]), axis=0)
        m_v[...] = new

    def head(*accs):
        def trip(i, carry):
            steps = [(b, k) for b in range(held + pair) for k in range(dim // 256)]

            def weights(b, at, k):
                lanes = slice(k * 256, (k + 1) * 256)
                if b < held:
                    return ring[pl.ds(pl.multiple_of((i * held + b) * BLOCK + at, 256), 256), lanes]
                return stream[b - held, at:at + 256, lanes]

            def push_w(j):
                b, k = steps[j]
                if b >= held and k == 0:
                    stream_copy(i, b - held).wait()
                for q in (0, 1):
                    pltpu.matmul_push_rhs(weights(b, q * 512, k), staging_register=0, mxu_index=q, transpose=True)

            def push_o(j):
                k = steps[j][1]
                for q in (0, 1):
                    pltpu.matmul_push_rhs(o_v[k * 256:(k + 1) * 256, :], staging_register=1, mxu_index=q, transpose=False)

            def pops(b):
                block = i * held + b if b < held else SLOTS + i * pair + b - held
                at = pl.multiple_of(block * BLOCK, BLOCK)
                for q in (0, 1):
                    block = jnp.transpose(pltpu.matmul_pop(accs[q * 4 + b % 2 * 2]))
                    z_ref[pl.ds(at + q * 512, 256), :] = block
                    fold(block)
                    block = pltpu.matmul_pop(accs[q * 4 + b % 2 * 2 + 1])[:, :rows]
                    z_ref[pl.ds(at + q * 512 + 256, 256), :] = block
                    fold(block)

            push_w(0)
            push_o(0)
            for j, (b, k) in enumerate(steps):
                for q in (0, 1):
                    pltpu.matmul_acc_lhs(accs[q * 4 + b % 2 * 2], o_rows[:, k * 256:(k + 1) * 256], load_staged_rhs=0)
                if j + 1 < len(steps):
                    push_w(j + 1)
                for q in (0, 1):
                    pltpu.matmul_acc_lhs(accs[q * 4 + b % 2 * 2 + 1], weights(b, q * 512 + 256, k), load_staged_rhs=1)
                if j + 1 < len(steps):
                    push_o(j + 1)
                if k == 2 and b > 0:
                    pops(b - 1)
            pops(held + pair - 1)

            @pl.when(i + 1 < trips)
            def _():
                for b in range(pair):
                    stream_copy(i + 1, b).start()
            return carry

        lax.fori_loop(0, trips, trip, 0)

    pl.run_scoped(head, *[pltpu.ACC(q)((size, 256), F32) for q in (0, 1) for _ in (0, 1) for size in (128, 256)])
    end_copy.wait()
    first_rows = rest // 32 * 16
    sizes = (first_rows, rest - first_rows)

    def tail(*accs):
        for k in range(dim // 256):
            for q in (0, 1):
                pltpu.matmul_push_rhs(o_v[k * 256:(k + 1) * 256, :], staging_register=k % 2, mxu_index=q, transpose=False)
                pltpu.matmul_acc_lhs(accs[q], end_v[q * sizes[0]:q * sizes[0] + sizes[q], k * 256:(k + 1) * 256], load_staged_rhs=k % 2)
        for q in (0, 1):
            block = pltpu.matmul_pop(accs[q])[:, :rows]
            z_ref[pl.ds(blocks * BLOCK + q * sizes[0], sizes[q]), :] = block
            fold(block)

    pl.run_scoped(tail, *[pltpu.ACC(q)((sizes[q], 256), F32) for q in (0, 1)])
    m_row = jnp.max(m_v[...], axis=0, keepdims=True)
    s_row = jnp.sum(s_v[...] * jnp.exp(m_v[...] - m_row), axis=0, keepdims=True)
    stat_ref[...] = jnp.concatenate([m_row, s_row, jnp.zeros((6, rows), F32)], axis=0)


def total_kernel(n, stat_ref, lse_ref, stat_in, send_sem, recv_sem):
    me = lax.axis_index("tp")
    barrier = pltpu.get_barrier_semaphore()
    for d in range(1, n):
        pl.semaphore_signal(barrier, inc=1, device_id={"tp": lax.rem(me + d, n)}, device_id_type=MESH)
    stat_in[me] = stat_ref[...]
    pl.semaphore_wait(barrier, n - 1)
    copies = []
    for d in (4, 6, 2, 3, 5, 7, 1):
        copies.append(pltpu.make_async_remote_copy(
            src_ref=stat_ref, dst_ref=stat_in.at[me], send_sem=send_sem.at[d - 1], recv_sem=recv_sem.at[d - 1],
            device_id={"tp": lax.rem(me + d, n)}, device_id_type=MESH))
        copies[-1].start()
    for copy in copies:
        copy.wait_recv()
    stats = stat_in[...]
    m_all, s_all = stats[:, 0, :], stats[:, 1, :]
    m_top = jnp.max(m_all, axis=0, keepdims=True)
    lse = m_top + jnp.log(jnp.sum(s_all * jnp.exp(m_all - m_top), axis=0, keepdims=True))
    lse_ref[...] = jnp.broadcast_to(lse, lse_ref.shape)
    for copy in copies:
        copy.wait_send()


def close_kernel(z_ref, lse_ref, u_in, logp_hbm, u_hbm, stage, u_stage, sem):
    vocab = z_ref.shape[0]
    copies = []
    for i, at in enumerate(range(0, vocab, CLOSE)):
        size = min(CLOSE, vocab - at)
        stage[at:at + size, :] = z_ref[at:at + size, :] - lse_ref[0:1, :]
        copies.append(pltpu.make_async_copy(stage.at[pl.ds(at, size), :], logp_hbm.at[pl.ds(at, size), :], sem.at[i]))
        copies[-1].start()
    u_stage[...] = jnp.transpose(u_in[...])
    copies.append(pltpu.make_async_copy(u_stage, u_hbm, sem.at[len(copies)]))
    copies[-1].start()
    for copy in copies:
        copy.wait()


def solution(mesh):
    n = mesh.shape["tp"]

    def draft_step(hidden, tokens, embedding, head_w, h_norm, e_norm, f_norm, o_norm, proj_w, w_gate, w_up, w_down):
        rows, dim = hidden.shape
        vocab = head_w.shape[1]
        cols, ffn = proj_w.shape[1], w_gate.shape[1]
        chunk = rows // n
        smem = pl.BlockSpec(memory_space=pltpu.SMEM)
        vmem = pl.BlockSpec(memory_space=pltpu.VMEM)
        hbm = pl.BlockSpec(memory_space=pl.ANY)
        dma = pltpu.SemaphoreType.DMA
        on_chip = functools.partial(pltpu.with_memory_space_constraint, memory_space=pltpu.VMEM)
        emb_rows = pl.pallas_call(
            gather_kernel,
            out_shape=jax.ShapeDtypeStruct((rows, dim), BF16),
            in_specs=[smem, vmem, hbm],
            out_specs=vmem,
            scratch_shapes=[pltpu.VMEM((rows * 8, dim), BF16), dma],
            compiler_params=pltpu.CompilerParams(vmem_limit_bytes=GATHER_MIB * 1024 * 1024),
            name="gather_rows",
        )(tokens, tokens[None, :], embedding)

        head_t = head_w.T
        ring, o_cols, o_rows, u = pl.pallas_call(
            functools.partial(main_kernel, n),
            out_shape=(pltpu.VMEM((SLOTS * BLOCK, dim), BF16), pltpu.VMEM((dim, rows), BF16), pltpu.VMEM((rows, dim), BF16),
                       pltpu.VMEM((dim, rows), BF16)),
            in_specs=[hbm] * 11,
            out_specs=(vmem, vmem, vmem, vmem),
            scratch_shapes=[
                pltpu.VMEM((rows, dim), BF16), pltpu.VMEM((rows, dim), BF16), *[pltpu.VMEM((dim,), F32)] * 4,
                pltpu.VMEM((cols, 2 * dim), BF16), pltpu.VMEM((ffn, dim), BF16), pltpu.VMEM((ffn, dim), BF16),
                pltpu.VMEM((dim, 2 * pl.cdiv(ffn, 128) * 128), BF16),
                pltpu.VMEM((ffn, dim), BF16),
                pltpu.VMEM((rows // 2, dim), BF16), pltpu.VMEM((3, chunk, dim), BF16),
                pltpu.VMEM((chunk, dim), BF16), pltpu.VMEM((rows, dim), BF16),
                pltpu.VMEM((cols, rows), BF16), pltpu.VMEM((dim, rows), BF16),
                pltpu.VMEM((4, 2 * cols, rows), F32), pltpu.VMEM((4, cols, rows), F32),
                pltpu.VMEM((3, cols, rows), F32),
                pltpu.VMEM((cols, rows), BF16), pltpu.VMEM((dim, rows), BF16), pltpu.VMEM((dim, rows), F32),
                dma((10,)), dma((SLOTS,)), dma((40,)), dma((40,)),
            ],
            compiler_params=pltpu.CompilerParams(
                collective_id=0, has_side_effects=True, vmem_limit_bytes=int(MAIN_MIB * 1024 * 1024)),
            name="draft_main",
        )(emb_rows, hidden, h_norm, e_norm, f_norm, o_norm, proj_w.T, w_gate.T, w_up.T, w_down, head_t)

        z, stat = pl.pallas_call(
            head_kernel,
            out_shape=(pltpu.VMEM((vocab, rows), F32), pltpu.VMEM((8, rows), F32)),
            in_specs=[vmem, vmem, vmem, hbm],
            out_specs=(vmem, vmem),
            scratch_shapes=[
                pltpu.VMEM((PAIR, BLOCK, dim), BF16), pltpu.VMEM((vocab % BLOCK, dim), BF16), pltpu.VMEM((dim, 2 * rows), BF16),
                pltpu.VMEM((8, rows), F32), pltpu.VMEM((8, rows), F32), dma((PAIR + 1,))],
            compiler_params=pltpu.CompilerParams(vmem_limit_bytes=int(HEAD_MIB * 1024 * 1024)),
            name="head",
        )(*map(on_chip, (ring, o_cols, o_rows)), head_t)

        lse = pl.pallas_call(
            functools.partial(total_kernel, n),
            out_shape=pltpu.VMEM((8, rows), F32),
            in_specs=[vmem],
            out_specs=vmem,
            scratch_shapes=[pltpu.VMEM((n, 8, rows), F32), dma((n - 1,)), dma((n - 1,))],
            compiler_params=pltpu.CompilerParams(collective_id=1, has_side_effects=True, vmem_limit_bytes=4 * 1024 * 1024),
            name="total",
        )(stat)

        logp, new_u = pl.pallas_call(
            close_kernel,
            out_shape=(jax.ShapeDtypeStruct((vocab, rows), F32), jax.ShapeDtypeStruct((rows, dim), BF16)),
            in_specs=[vmem, vmem, vmem],
            out_specs=(hbm, hbm),
            scratch_shapes=[pltpu.VMEM((vocab, rows), F32), pltpu.VMEM((rows, dim), BF16), dma((pl.cdiv(vocab, CLOSE) + 1,))],
            compiler_params=pltpu.CompilerParams(vmem_limit_bytes=16 * 1024 * 1024),
            name="close",
        )(z, lse, u)
        return new_u, logp.T

    specs_in = (P("dp", None), P("dp"), P("tp", None), P(None, "tp"), P(None), P(None), P(None), P(None), P(None, "tp"), P(None, "tp"), P(None, "tp"), P("tp", None))
    specs_out = (P("dp", None), P("dp", "tp"))
    return jax.shard_map(draft_step, mesh=mesh, in_specs=specs_in, out_specs=specs_out, check_vma=False)
```

```python
import functools

import jax
import jax.numpy as jnp
from jax import lax
from jax.experimental import pallas as pl
from jax.experimental.pallas import tpu as pltpu
from jax.sharding import PartitionSpec as P

NORM_EPS = 1e-6
BLOCK = 1024
SLOTS = 10
MAIN_MIB = 23.4
PAIR = 4
HEAD_MIB = 23.4
GATHER_MIB = 60
CLOSE = 1024
MESH = pl.DeviceIdType.MESH
F32, BF16 = jnp.float32, jnp.bfloat16


def rms(values, gain, axis):
    wide = values.astype(F32)
    inv = lax.rsqrt(jnp.mean(wide * wide, axis=axis, keepdims=True) + NORM_EPS)
    return wide * inv * gain


def dot_t(a, b):
    return lax.dot_general(a, b, (((1,), (1,)), ((), ())), preferred_element_type=F32)


def gather_kernel(ids_ref, ids_row_ref, emb_hbm, emb_ref, buf, sem):
    rows = emb_ref.shape[0]
    vocab = emb_hbm.shape[0]
    base = lax.axis_index("tp") * vocab

    def issue(r, carry):
        local = ids_ref[r] - base
        local = jnp.where((local >= 0) & (local < vocab), local, r * 8)
        start = pl.multiple_of((local // 8) * 8, 8)
        pltpu.make_async_copy(emb_hbm.at[pl.ds(start, 8), :], buf.at[pl.ds(pl.multiple_of(r * 8, 8), 8), :], sem).start()
        return carry

    lax.fori_loop(0, rows, issue, 0, unroll=16)
    local = ids_row_ref[...] - base
    owned = (local >= 0) & (local < vocab)
    want = lax.broadcasted_iota(jnp.int32, (rows * 8, rows), 1) * 8 + (local & 7)
    here = lax.broadcasted_iota(jnp.int32, (rows * 8, rows), 0)
    pick = jnp.where((here == want) & owned, 1.0, 0.0).astype(BF16)
    pltpu.make_async_copy(emb_hbm.at[pl.ds(0, rows * 8), :], buf, sem).wait()
    emb_ref[...] = lax.dot_general(pick, buf[...], (((0,), (0,)), ((), ())), preferred_element_type=F32).astype(BF16)


def main_kernel(n, emb_hbm, hid_hbm, h_hbm, e_hbm, f_hbm, o_hbm,
                proj_hbm, gate_hbm, up_hbm, down_hbm, head_hbm,
                ring, o_v, o_rows, u_ref,
                emb_ref, hid_ref, h_gain, e_gain, f_gain, o_gain, proj_v, gate_v, up_v, wide_w, down_v, emb_pair, emb_in, emb_mine, emb_all, p_mine, p_all,
                part_v, pair_in, part_in, u_mine, u_all, wide,
                w_sem, ring_sem, send_sem, recv_sem):
    me = lax.axis_index("tp")
    rows, dim = hid_ref.shape
    chunk = rows // n
    cols, ffn = p_mine.shape[0], gate_hbm.shape[0]

    core, chip = lax.rem(me, 2), lax.div(me, 2)
    partner = me + 1 - 2 * core
    x, y = lax.rem(chip, 2), lax.div(chip, 2)
    chips = (chip, chip + 1 - 2 * x, chip + 2 - 4 * y, 3 - chip)
    far = (3, 1, 2)

    local = [pltpu.make_async_copy(src, dst, w_sem.at[4 + i]) for i, (src, dst) in enumerate((
        (emb_hbm, emb_ref), (hid_hbm, hid_ref), (h_hbm, h_gain), (e_hbm, e_gain), (f_hbm, f_gain), (o_hbm, o_gain)))]
    for copy in local:
        copy.start()
    weights = [pltpu.make_async_copy(src, dst, w_sem.at[i]) for i, (src, dst) in enumerate(
        ((proj_hbm, proj_v), (gate_hbm, gate_v), (up_hbm, up_v), (down_hbm, down_v)))]
    for copy in weights:
        copy.start()

    def head_copy(t):
        at = pl.ds(pl.multiple_of(t * BLOCK, BLOCK), BLOCK)
        return pltpu.make_async_copy(head_hbm.at[at, :], ring.at[at, :], ring_sem.at[t])

    barrier = pltpu.get_barrier_semaphore()
    for d in range(1, n):
        pl.semaphore_signal(barrier, inc=1, device_id={"tp": lax.rem(me + d, n)}, device_id_type=MESH)
    local[0].wait()
    pl.semaphore_wait(barrier, n - 1)

    sent = []

    def send(source, target, device):
        i = len(sent)
        copy = pltpu.make_async_remote_copy(src_ref=source, dst_ref=target, send_sem=send_sem.at[i], recv_sem=recv_sem.at[i],
                                            device_id={"tp": device}, device_id_type=MESH)
        copy.start()
        sent.append(copy)
        return copy

    def part(ref, j, size):
        return ref.at[pl.ds(pl.multiple_of(j * size, size), size), :]

    def all_gather(mine, place, meanwhile=lambda: None):
        beside = [send(mine, place(me), partner)]
        arriving = {m: send(mine, place(me), chips[m] * 2 + core) for m in far}
        place(me)[...] = mine[...]
        meanwhile()
        for m in (1, 2, 3):
            arriving[m].wait_recv()
            there = place(chips[m] * 2 + core)
            beside.append(send(there, there, partner))
        for copy in beside:
            copy.wait_recv()

    pairs = {m: send(part(emb_ref, (1 - core) * (n // 2) + chips[m], chunk), emb_pair.at[m], partner) for m in (3, 2, 1, 0)}

    def prefetch(t, carry):
        head_copy(t).start()
        return carry

    lax.fori_loop(0, SLOTS, prefetch, 0)
    for copy in local[1:]:
        copy.wait()
    hid_ref[...] = rms(hid_ref[...], h_gain[...][None, :], -1).astype(BF16)
    first = []
    for m in (3, 2, 1, 0):
        pairs[m].wait_recv()
        block = part(emb_ref, core * (n // 2) + chips[m], chunk)
        block[...] = block[...] + emb_pair[m]
        if m:
            first.append(send(block, emb_in.at[m - 1], chips[m] * 2 + core))
    turned = pl.cdiv(ffn, 128) * 128

    def turn(i, begin, end):
        source = (gate_v, up_v)[i]
        for at in range(begin, end, 256):
            size = min(256, end - at)
            wide_w[:, i * turned + at:i * turned + at + size] = jnp.transpose(source[at:at + size, :])

    weights[0].wait()
    acc_h = dot_t(proj_v[:, :dim], hid_ref[...])
    wide[...] = jnp.transpose(jnp.broadcast_to(f_gain[...][None, :], (rows, dim)))
    weights[1].wait()
    turn(0, 0, ffn)
    weights[2].wait()
    total = part(emb_ref, core * (n // 2) + chip, chunk)[...].astype(F32)
    for copy in first:
        copy.wait_recv()
    for m in (0, 1, 2):
        total = total + emb_in[m].astype(F32)
    emb_mine[...] = rms(total, e_gain[...][None, :], -1).astype(BF16)
    all_gather(emb_mine, lambda j: part(emb_all, lax.rem(j, 2) * (n // 2) + lax.div(j, 2), chunk), lambda: turn(1, 0, 512))
    p_mine[...] = (acc_h + dot_t(proj_v[:, dim:], emb_all[...])).astype(BF16)

    all_gather(p_mine, lambda j: part(p_all, j, cols), lambda: turn(1, 512, ffn))
    normed = rms(p_all[...], wide[...], 0).astype(BF16)
    hidden = jnp.dot(jnp.transpose(normed), wide_w[...], preferred_element_type=F32)
    act = (jax.nn.silu(hidden[:, :ffn]) * hidden[:, turned:turned + ffn]).astype(BF16)
    weights[3].wait()

    mine = pl.ds(pl.multiple_of(core * cols, cols), cols)
    other = pl.ds(pl.multiple_of((1 - core) * cols, cols), cols)
    pairs, arriving = {}, []

    def narrow(m):
        columns = pl.ds(pl.multiple_of(chips[m] * 2 * cols, 2 * cols), 2 * cols)
        part_v[m] = jnp.transpose(jnp.dot(act, down_v[:, columns], preferred_element_type=F32))
        pairs[m] = send(part_v.at[m, other, :], pair_in.at[m], partner)

    def pass_on(m):
        pairs[m].wait_recv()
        part_v[m, mine, :] = part_v[m, mine, :] + pair_in[m]
        arriving.append(send(part_v.at[m, mine, :], part_in.at[m - 1], chips[m] * 2 + core))

    narrow(2)
    narrow(3)
    narrow(1)
    pass_on(2)
    pass_on(3)
    narrow(0)
    pass_on(1)
    pairs[0].wait_recv()
    total = part_v[0, mine, :] + pair_in[0]
    wide[...] = jnp.transpose(jnp.broadcast_to(o_gain[...][None, :], (rows, dim)))
    for copy in arriving:
        copy.wait_recv()
    for m in (0, 1, 2):
        total = total + part_in[m]
    u_mine[...] = (p_mine[...].astype(F32) + total).astype(BF16)
    all_gather(u_mine, lambda j: part(u_all, j, cols))
    normed_o = rms(u_all[...], wide[...], 0).astype(BF16)
    o_v[...] = normed_o
    o_rows[...] = jnp.transpose(normed_o)
    u_ref[...] = u_all[...]

    def drain(t, carry):
        head_copy(t).wait()
        return carry

    lax.fori_loop(0, SLOTS, drain, 0)
    for copy in sent:
        copy.wait_send()


def head_kernel(ring, o_in, o_rows, head_hbm, z_ref, stat_ref, stream, end_v, o_v, m_v, s_v, stream_sem):
    rows, dim = o_rows.shape
    vocab = head_hbm.shape[0]
    blocks = vocab // BLOCK
    rest = vocab - blocks * BLOCK
    pair = stream.shape[0]
    trips = (blocks - SLOTS) // pair
    held = SLOTS // trips

    def stream_copy(t, b):
        at = pl.multiple_of((SLOTS + t * pair + b) * BLOCK, BLOCK)
        return pltpu.make_async_copy(head_hbm.at[pl.ds(at, BLOCK), :], stream.at[b], stream_sem.at[b])

    end_copy = pltpu.make_async_copy(head_hbm.at[pl.ds(blocks * BLOCK, rest), :], end_v, stream_sem.at[pair])
    for b in range(pair):
        stream_copy(0, b).start()
    end_copy.start()
    o_v[:, :rows] = o_in[...]
    o_v[:, rows:] = jnp.zeros_like(o_in[...])

    m_v[...] = jnp.full_like(m_v, -jnp.inf)
    s_v[...] = jnp.zeros_like(s_v)

    def fold(block):
        groups = block.reshape(block.shape[0] // 8, 8, rows)
        old = m_v[...]
        new = jnp.maximum(old, jnp.max(groups, axis=0))
        s_v[...] = s_v[...] * jnp.exp(old - new) + jnp.sum(jnp.exp(groups - new[None]), axis=0)
        m_v[...] = new

    def head(*accs):
        def trip(i, carry):
            steps = [(b, k) for b in range(held + pair) for k in range(dim // 256)]

            def weights(b, at, k):
                lanes = slice(k * 256, (k + 1) * 256)
                if b < held:
                    return ring[pl.ds(pl.multiple_of((i * held + b) * BLOCK + at, 256), 256), lanes]
                return stream[b - held, at:at + 256, lanes]

            def push_w(j):
                b, k = steps[j]
                if b >= held and k == 0:
                    stream_copy(i, b - held).wait()
                for q in (0, 1):
                    pltpu.matmul_push_rhs(weights(b, q * 512, k), staging_register=0, mxu_index=q, transpose=True)

            def push_o(j):
                k = steps[j][1]
                for q in (0, 1):
                    pltpu.matmul_push_rhs(o_v[k * 256:(k + 1) * 256, :], staging_register=1, mxu_index=q, transpose=False)

            def pops(b):
                block = i * held + b if b < held else SLOTS + i * pair + b - held
                at = pl.multiple_of(block * BLOCK, BLOCK)
                for q in (0, 1):
                    block = jnp.transpose(pltpu.matmul_pop(accs[q * 4 + b % 2 * 2]))
                    z_ref[pl.ds(at + q * 512, 256), :] = block
                    fold(block)
                    block = pltpu.matmul_pop(accs[q * 4 + b % 2 * 2 + 1])[:, :rows]
                    z_ref[pl.ds(at + q * 512 + 256, 256), :] = block
                    fold(block)

            push_w(0)
            push_o(0)
            for j, (b, k) in enumerate(steps):
                for q in (0, 1):
                    pltpu.matmul_acc_lhs(accs[q * 4 + b % 2 * 2], o_rows[:, k * 256:(k + 1) * 256], load_staged_rhs=0)
                if j + 1 < len(steps):
                    push_w(j + 1)
                for q in (0, 1):
                    pltpu.matmul_acc_lhs(accs[q * 4 + b % 2 * 2 + 1], weights(b, q * 512 + 256, k), load_staged_rhs=1)
                if j + 1 < len(steps):
                    push_o(j + 1)
                if k == 2 and b > 0:
                    pops(b - 1)
            pops(held + pair - 1)

            @pl.when(i + 1 < trips)
            def _():
                for b in range(pair):
                    stream_copy(i + 1, b).start()
            return carry

        lax.fori_loop(0, trips, trip, 0)

    pl.run_scoped(head, *[pltpu.ACC(q)((size, 256), F32) for q in (0, 1) for _ in (0, 1) for size in (128, 256)])
    end_copy.wait()
    first_rows = rest // 32 * 16
    sizes = (first_rows, rest - first_rows)

    def tail(*accs):
        for k in range(dim // 256):
            for q in (0, 1):
                pltpu.matmul_push_rhs(o_v[k * 256:(k + 1) * 256, :], staging_register=k % 2, mxu_index=q, transpose=False)
                pltpu.matmul_acc_lhs(accs[q], end_v[q * sizes[0]:q * sizes[0] + sizes[q], k * 256:(k + 1) * 256], load_staged_rhs=k % 2)
        for q in (0, 1):
            block = pltpu.matmul_pop(accs[q])[:, :rows]
            z_ref[pl.ds(blocks * BLOCK + q * sizes[0], sizes[q]), :] = block
            fold(block)

    pl.run_scoped(tail, *[pltpu.ACC(q)((sizes[q], 256), F32) for q in (0, 1)])
    m_row = jnp.max(m_v[...], axis=0, keepdims=True)
    s_row = jnp.sum(s_v[...] * jnp.exp(m_v[...] - m_row), axis=0, keepdims=True)
    stat_ref[...] = jnp.concatenate([m_row, s_row, jnp.zeros((6, rows), F32)], axis=0)


def total_kernel(n, stat_ref, lse_ref, stat_in, send_sem, recv_sem):
    me = lax.axis_index("tp")
    barrier = pltpu.get_barrier_semaphore()
    for d in range(1, n):
        pl.semaphore_signal(barrier, inc=1, device_id={"tp": lax.rem(me + d, n)}, device_id_type=MESH)
    stat_in[me] = stat_ref[...]
    pl.semaphore_wait(barrier, n - 1)
    copies = []
    for d in (4, 6, 2, 3, 5, 7, 1):
        copies.append(pltpu.make_async_remote_copy(
            src_ref=stat_ref, dst_ref=stat_in.at[me], send_sem=send_sem.at[d - 1], recv_sem=recv_sem.at[d - 1],
            device_id={"tp": lax.rem(me + d, n)}, device_id_type=MESH))
        copies[-1].start()
    for copy in copies:
        copy.wait_recv()
    stats = stat_in[...]
    m_all, s_all = stats[:, 0, :], stats[:, 1, :]
    m_top = jnp.max(m_all, axis=0, keepdims=True)
    lse = m_top + jnp.log(jnp.sum(s_all * jnp.exp(m_all - m_top), axis=0, keepdims=True))
    lse_ref[...] = jnp.broadcast_to(lse, lse_ref.shape)
    for copy in copies:
        copy.wait_send()


def close_kernel(z_ref, lse_ref, u_in, logp_hbm, u_hbm, stage, u_stage, sem):
    vocab = z_ref.shape[0]
    copies = []
    for i, at in enumerate(range(0, vocab, CLOSE)):
        size = min(CLOSE, vocab - at)
        stage[at:at + size, :] = z_ref[at:at + size, :] - lse_ref[0:1, :]
        copies.append(pltpu.make_async_copy(stage.at[pl.ds(at, size), :], logp_hbm.at[pl.ds(at, size), :], sem.at[i]))
        copies[-1].start()
    u_stage[...] = jnp.transpose(u_in[...])
    copies.append(pltpu.make_async_copy(u_stage, u_hbm, sem.at[len(copies)]))
    copies[-1].start()
    for copy in copies:
        copy.wait()


def solution(mesh):
    n = mesh.shape["tp"]

    def draft_step(hidden, tokens, embedding, head_w, h_norm, e_norm, f_norm, o_norm, proj_w, w_gate, w_up, w_down):
        rows, dim = hidden.shape
        vocab = head_w.shape[1]
        cols, ffn = proj_w.shape[1], w_gate.shape[1]
        chunk = rows // n
        smem = pl.BlockSpec(memory_space=pltpu.SMEM)
        vmem = pl.BlockSpec(memory_space=pltpu.VMEM)
        hbm = pl.BlockSpec(memory_space=pl.ANY)
        dma = pltpu.SemaphoreType.DMA
        on_chip = functools.partial(pltpu.with_memory_space_constraint, memory_space=pltpu.VMEM)
        emb_rows = pl.pallas_call(
            gather_kernel,
            out_shape=jax.ShapeDtypeStruct((rows, dim), BF16),
            in_specs=[smem, vmem, hbm],
            out_specs=vmem,
            scratch_shapes=[pltpu.VMEM((rows * 8, dim), BF16), dma],
            compiler_params=pltpu.CompilerParams(vmem_limit_bytes=GATHER_MIB * 1024 * 1024),
            name="gather_rows",
        )(tokens, tokens[None, :], embedding)

        head_t = head_w.T
        ring, o_cols, o_rows, u = pl.pallas_call(
            functools.partial(main_kernel, n),
            out_shape=(pltpu.VMEM((SLOTS * BLOCK, dim), BF16), pltpu.VMEM((dim, rows), BF16), pltpu.VMEM((rows, dim), BF16),
                       pltpu.VMEM((dim, rows), BF16)),
            in_specs=[hbm] * 11,
            out_specs=(vmem, vmem, vmem, vmem),
            scratch_shapes=[
                pltpu.VMEM((rows, dim), BF16), pltpu.VMEM((rows, dim), BF16), *[pltpu.VMEM((dim,), F32)] * 4,
                pltpu.VMEM((cols, 2 * dim), BF16), pltpu.VMEM((ffn, dim), BF16), pltpu.VMEM((ffn, dim), BF16),
                pltpu.VMEM((dim, 2 * pl.cdiv(ffn, 128) * 128), BF16),
                pltpu.VMEM((ffn, dim), BF16),
                pltpu.VMEM((4, chunk, dim), BF16), pltpu.VMEM((3, chunk, dim), BF16),
                pltpu.VMEM((chunk, dim), BF16), pltpu.VMEM((rows, dim), BF16),
                pltpu.VMEM((cols, rows), BF16), pltpu.VMEM((dim, rows), BF16),
                pltpu.VMEM((4, 2 * cols, rows), F32), pltpu.VMEM((4, cols, rows), F32),
                pltpu.VMEM((3, cols, rows), F32),
                pltpu.VMEM((cols, rows), BF16), pltpu.VMEM((dim, rows), BF16), pltpu.VMEM((dim, rows), F32),
                dma((10,)), dma((SLOTS,)), dma((40,)), dma((40,)),
            ],
            compiler_params=pltpu.CompilerParams(
                collective_id=0, has_side_effects=True, vmem_limit_bytes=int(MAIN_MIB * 1024 * 1024)),
            name="draft_main",
        )(emb_rows, hidden, h_norm, e_norm, f_norm, o_norm, proj_w.T, w_gate.T, w_up.T, w_down, head_t)

        z, stat = pl.pallas_call(
            head_kernel,
            out_shape=(pltpu.VMEM((vocab, rows), F32), pltpu.VMEM((8, rows), F32)),
            in_specs=[vmem, vmem, vmem, hbm],
            out_specs=(vmem, vmem),
            scratch_shapes=[
                pltpu.VMEM((PAIR, BLOCK, dim), BF16), pltpu.VMEM((vocab % BLOCK, dim), BF16), pltpu.VMEM((dim, 2 * rows), BF16),
                pltpu.VMEM((8, rows), F32), pltpu.VMEM((8, rows), F32), dma((PAIR + 1,))],
            compiler_params=pltpu.CompilerParams(vmem_limit_bytes=int(HEAD_MIB * 1024 * 1024)),
            name="head",
        )(*map(on_chip, (ring, o_cols, o_rows)), head_t)

        lse = pl.pallas_call(
            functools.partial(total_kernel, n),
            out_shape=pltpu.VMEM((8, rows), F32),
            in_specs=[vmem],
            out_specs=vmem,
            scratch_shapes=[pltpu.VMEM((n, 8, rows), F32), dma((n - 1,)), dma((n - 1,))],
            compiler_params=pltpu.CompilerParams(collective_id=1, has_side_effects=True, vmem_limit_bytes=4 * 1024 * 1024),
            name="total",
        )(stat)

        logp, new_u = pl.pallas_call(
            close_kernel,
            out_shape=(jax.ShapeDtypeStruct((vocab, rows), F32), jax.ShapeDtypeStruct((rows, dim), BF16)),
            in_specs=[vmem, vmem, vmem],
            out_specs=(hbm, hbm),
            scratch_shapes=[pltpu.VMEM((vocab, rows), F32), pltpu.VMEM((rows, dim), BF16), dma((pl.cdiv(vocab, CLOSE) + 1,))],
            compiler_params=pltpu.CompilerParams(vmem_limit_bytes=16 * 1024 * 1024),
            name="close",
        )(z, lse, u)
        return new_u, logp.T

    specs_in = (P("dp", None), P("dp"), P("tp", None), P(None, "tp"), P(None), P(None), P(None), P(None), P(None, "tp"), P(None, "tp"), P(None, "tp"), P("tp", None))
    specs_out = (P("dp", None), P("dp", "tp"))
    return jax.shard_map(draft_step, mesh=mesh, in_specs=specs_in, out_specs=specs_out, check_vma=False)
```
